32 devices in a mesh: groups: 2 (over y), seg: 4 (over z), bin: 4 (over x, core).
Axes of the slice: x: 2, y: 2, z: 4, core: 2. Of those that a mesh axis runs over, the one named last changes fastest.
Arguments:
- start_factors: float32 [4096, 128], P(('groups', 'seg', 'bin')), parts along dimension 0, may hold values from -6 to 6
- bin_factors: bfloat16 [8192, 128], P(('groups', 'bin')), parts along dimension 0, may hold values from -0.5 to 0.5
- tile_speed: bfloat16 [8, 4, 12, 128, 128], P(('groups', 'seg'), 'bin'), parts along dimension 0, may hold values from -6 to 6
- tile_weight: bfloat16 [8, 4, 12, 128, 128], P(('groups', 'seg'), 'bin'), parts along dimension 0, may hold values from 0.099609375 to 2
- tile_cells: int32 [8, 4, 12, 2], P(('groups', 'seg'), 'bin'), parts along dimension 0, may hold values from 0 to 7, as said below
- tile_count: int32 [8, 4], P(('groups', 'seg'), 'bin'), parts along dimension 0, may hold values from 1 to 12, as said below
- inner_pairs: int32 [8, 4, 2, 2], P(('groups', 'seg'), 'bin'), parts along dimension 0, may hold values from 0 to 3, as said below
- inner_weight: float32 [8, 4, 2, 128, 128], P(('groups', 'seg'), 'bin'), parts along dimension 0, may hold values from 0 to 0.00390625
- face_rows: int32 [8, 4, 2, 256], P(('groups', 'seg'), 'bin'), parts along dimension 0, may hold values from 0 to 511, as said below
- face_count: int32 [8, 4, 2], P(('groups', 'seg'), 'bin'), parts along dimension 0, may hold values from 128 to 256, as said below
- face_weight: float32 [8, 4, 256, 256], P(('groups', 'seg'), 'bin'), parts along dimension 0, may hold values from 0 to 0.00390625
Outputs:
- solution_factors: float32 [4096, 128], P(('groups', 'seg', 'bin')), parts along dimension 0
- residual: float32 [4096, 128], P(('groups', 'seg', 'bin')), parts along dimension 0
The draws below stay inside these ranges and needn't reach their ends.
There are 2 independent parts, one for each index of `groups`. The reference program is written for one: setup_inputs(seed, part) draws one part's arguments, and reference() takes and returns one part's arrays. A program takes and returns all parts, laid end to end along the dimension named above; each array names one. Nothing has to cross between parts.
Inputs may be any that keep to these rules, and one draw needn't show every extreme that they name: `tile_cells`: the 12 slots of one device name different pairs; the first entry is a segment block of the partition, the second a bin block of the device's bins. `tile_count`: some device of every draw has all 12 slots live. `inner_pairs`: the two blocks of a pair differ; both are segment blocks of the partition. `face_rows`: row numbers within the partition, different within each face list. `face_count`: some face list of every draw has all 256 rows live.
All inputs are finite; a program needn't handle non-finite values.
Results may differ from the reference program's by a relative error of at most 0.0024.
Values sent between devices are 32-bit elements; how exact they have to be, the bound alone decides.
No kernel may reach another device: no remote copies, remote signals or barrier semaphores. Data moves between devices by JAX's collectives and lax.ppermute only.
A program may use at most 64 MiB of HBM per device.

```python
import jax
import jax.numpy as jnp
from jax import lax

TILE = 128
R = 128
SEGBLK_DEV = 4
BINBLK_DEV = 8
HR = 256
ITERS = 2
NT_DEV = 12
NI = 2
SEGS = 2048
BINS = 4096
N_SEG = 4
N_BIN = 4


def draw_tile_count(key, part):
    key_one, key_two, key_three = jax.random.split(key, 3)
    first = jax.random.randint(key_one, (N_SEG * N_BIN,), 0, NT_DEV)
    second = jax.random.randint(key_two, (N_SEG * N_BIN,), 0, NT_DEV)
    counts = 1 + first * second // NT_DEV
    chosen = jax.random.randint(key_three, (), 0, N_SEG * N_BIN)
    counts = jnp.where(jnp.arange(N_SEG * N_BIN) == chosen, NT_DEV, counts)
    return counts.reshape(N_SEG, N_BIN).astype(jnp.int32)


def draw_tile_cells(key, part):
    key_list = jax.random.split(key, N_SEG * N_BIN)
    shuffled = jax.vmap(lambda single: jax.random.permutation(single, SEGBLK_DEV * BINBLK_DEV)[:NT_DEV])(key_list)
    cells = jnp.stack([shuffled // BINBLK_DEV, shuffled % BINBLK_DEV], axis=-1)
    return cells.reshape(N_SEG, N_BIN, NT_DEV, 2).astype(jnp.int32)


def draw_inner_pairs(key, part):
    key_one, key_two = jax.random.split(key)
    first = jax.random.randint(key_one, (N_SEG, N_BIN, NI), 0, SEGBLK_DEV)
    offset = jax.random.randint(key_two, (N_SEG, N_BIN, NI), 1, SEGBLK_DEV)
    second = (first + offset) % SEGBLK_DEV
    return jnp.stack([first, second], axis=-1).astype(jnp.int32)


def draw_face_rows(key, part):
    key_list = jax.random.split(key, N_SEG * N_BIN * 2)
    shuffled = jax.vmap(lambda single: jax.random.permutation(single, TILE * SEGBLK_DEV)[:HR])(key_list)
    return shuffled.reshape(N_SEG, N_BIN, 2, HR).astype(jnp.int32)


def draw_face_count(key, part):
    key_one, key_two = jax.random.split(key)
    halfway = HR // 2
    counts = halfway + jax.random.randint(key_one, (N_SEG * N_BIN * 2,), 0, HR - halfway + 1)
    chosen = jax.random.randint(key_two, (), 0, N_SEG * N_BIN * 2)
    counts = jnp.where(jnp.arange(N_SEG * N_BIN * 2) == chosen, HR, counts)
    return counts.reshape(N_SEG, N_BIN, 2).astype(jnp.int32)


def steps_of(own_key, dims, pieces, least, largest):
    def one(dim, parts):
        steps = jax.random.uniform(jax.random.fold_in(jax.random.fold_in(own_key, 6), dim), (parts,), jnp.float32, least / len(pieces), largest / len(pieces))
        return jnp.repeat(jnp.exp(steps), dims[dim] // parts).reshape((-1,) + (1,) * (len(dims) - dim - 1))

    gain = one(*pieces[0])
    for cut in pieces[1:]:
        gain = gain * one(*cut)
    return gain


def noise(own_key, shape, spread, most, cuts=(), kind=jnp.bfloat16):
    array = spread * jax.random.normal(own_key, shape, jnp.float32)
    if cuts:
        array = array * steps_of(own_key, shape, cuts, -0.22, 0.18)
    return jnp.clip(array, -most, most).astype(kind)


def setup_inputs(seed: int = 0, part: int = 0) -> dict:
    keys = jax.random.split(jax.random.key(seed), 12)
    part_splits = jax.random.split(jax.random.fold_in(keys[11], part), 12)
    return {
        "start_factors": noise(part_splits[0], (SEGS, R), 1.0, 6.0, ((0, 16),), jnp.float32),
        "bin_factors": noise(part_splits[1], (BINS, R), R ** -0.5, 0.5, ((0, 4),)),
        "tile_speed": noise(part_splits[2], (N_SEG, N_BIN, NT_DEV, TILE, TILE), 1.0, 6.0, ((0, 4), (1, 4))),
        "tile_weight": jnp.clip(0.099609375 + 1.9003906 * jax.random.uniform(part_splits[3], (N_SEG, N_BIN, NT_DEV, TILE, TILE), jnp.float32) ** steps_of(part_splits[3], (N_SEG, N_BIN, NT_DEV, TILE, TILE), ((0, 4), (1, 4)), -0.2, 0.2), 0.099609375, 2.0).astype(jnp.bfloat16),
        "tile_cells": draw_tile_cells(jax.random.fold_in(jax.random.fold_in(keys[11], part), 71), part),
        "tile_count": draw_tile_count(jax.random.fold_in(jax.random.fold_in(keys[11], part), 71), part),
        "inner_pairs": draw_inner_pairs(jax.random.fold_in(jax.random.fold_in(keys[11], part), 71), part),
        "inner_weight": jnp.clip(0.00390625 * jax.random.uniform(part_splits[7], (N_SEG, N_BIN, NI, TILE, TILE), jnp.float32) ** steps_of(part_splits[7], (N_SEG, N_BIN, NI, TILE, TILE), ((0, 4), (1, 4)), -0.2, 0.2), 0.0, 0.00390625),
        "face_rows": draw_face_rows(jax.random.fold_in(jax.random.fold_in(keys[11], part), 71), part),
        "face_count": draw_face_count(jax.random.fold_in(jax.random.fold_in(keys[11], part), 71), part),
        "face_weight": jnp.clip(0.00390625 * jax.random.uniform(part_splits[10], (N_SEG, N_BIN, HR, HR), jnp.float32) ** steps_of(part_splits[10], (N_SEG, N_BIN, HR, HR), ((0, 4), (1, 4)), -0.2, 0.2), 0.0, 0.00390625),
    }


highest = lax.Precision.HIGHEST
ridge_weight = 0.5


def tile_image(factors, bin_factors, tile_cells, tile_count, tile_weight):
    blocks_all = factors.reshape(N_SEG, SEGBLK_DEV, TILE, R)
    bins_all = bin_factors.astype(jnp.float32).reshape(N_BIN, BINBLK_DEV, TILE, R)
    bin_index = jnp.arange(N_BIN, dtype=jnp.int32)[:, None]
    slot_index = jnp.arange(NT_DEV, dtype=jnp.int32)[None, :]

    def one_part(packed):
        blocks, cells, counts, weights = packed
        picked = blocks[cells[:, :, 0]]
        chosen = bins_all[bin_index, cells[:, :, 1]]
        live_tiles = (slot_index < counts[:, None]).astype(jnp.float32)
        tile_gain = weights.astype(jnp.float32) * live_tiles[:, :, None, None]
        scores = jnp.einsum("tkir,tkjr->tkij", picked, chosen, precision=highest) * tile_gain
        pulled = jnp.einsum("tkij,tkjr->tkir", scores, chosen, precision=highest)
        return jnp.zeros((SEGBLK_DEV, TILE, R), jnp.float32).at[cells[:, :, 0]].add(pulled)

    return lax.map(one_part, (blocks_all, tile_cells, tile_count, tile_weight)).reshape(-1, R)


def right_side(bin_factors, tile_speed, tile_weight, tile_cells, tile_count):
    bins_all = bin_factors.reshape(N_BIN, BINBLK_DEV, TILE, R)
    bin_index = jnp.arange(N_BIN, dtype=jnp.int32)[:, None]
    slot_index = jnp.arange(NT_DEV, dtype=jnp.int32)[None, :]

    def one_part(packed):
        speeds, weights, cells, counts = packed
        chosen = bins_all[bin_index, cells[:, :, 1]].astype(jnp.float32)
        weighted = (weights.astype(jnp.float32) * speeds.astype(jnp.float32)).astype(jnp.bfloat16)
        live_tiles = (slot_index < counts[:, None]).astype(jnp.float32)
        terms = jnp.einsum("tkij,tkjr->tkir", weighted.astype(jnp.float32), chosen, precision=highest)
        terms = terms * live_tiles[:, :, None, None]
        return jnp.zeros((SEGBLK_DEV, TILE, R), jnp.float32).at[cells[:, :, 0]].add(terms)

    return lax.map(one_part, (tile_speed, tile_weight, tile_cells, tile_count)).reshape(-1, R)


def inner_image(factors, inner_pairs, inner_weight):
    blocks = factors.reshape(N_SEG, SEGBLK_DEV, TILE, R)
    part_index = jnp.arange(N_SEG, dtype=jnp.int32)[:, None, None]
    left = blocks[part_index, inner_pairs[..., 0]]
    right = blocks[part_index, inner_pairs[..., 1]]
    to_left = inner_weight.sum(4)[..., None] * left - jnp.einsum("stkij,stkjr->stkir", inner_weight, right, precision=highest)
    to_right = inner_weight.sum(3)[..., None] * right - jnp.einsum("stkij,stkir->stkjr", inner_weight, left, precision=highest)
    summed = jnp.zeros_like(blocks).at[part_index, inner_pairs[..., 0]].add(to_left)
    summed = summed.at[part_index, inner_pairs[..., 1]].add(to_right)
    return summed.reshape(-1, R)


def face_image(factors, face_rows, face_count, face_weight):
    part_rows = factors.reshape(N_SEG, SEGBLK_DEV * TILE, R)
    part_index = jnp.arange(N_SEG, dtype=jnp.int32)[:, None, None]
    slots = jnp.arange(HR, dtype=jnp.int32)[None, None, :]
    rows_low = face_rows[:, :, 0]
    rows_up = face_rows[:, :, 1]
    mask_low = (slots < face_count[:, :, 0:1]).astype(jnp.float32)
    mask_up = (slots < face_count[:, :, 1:2]).astype(jnp.float32)
    own_face = part_rows[part_index, rows_low] * mask_low[..., None]
    upper_face = part_rows[part_index, rows_up] * mask_up[..., None]
    lower_face = jnp.concatenate([jnp.zeros_like(upper_face[:1]), upper_face[:-1]], axis=0)
    lower_mask = jnp.concatenate([jnp.zeros_like(mask_up[:1]), mask_up[:-1]], axis=0)
    coupling = face_weight * mask_low[..., :, None] * lower_mask[..., None, :]
    own_term = coupling.sum(3)[..., None] * own_face - jnp.einsum("stij,stjr->stir", coupling, lower_face, precision=highest)
    answer = coupling.sum(2)[..., None] * lower_face - jnp.einsum("stij,stir->stjr", coupling, own_face, precision=highest)
    returned = jnp.concatenate([answer[1:], jnp.zeros_like(answer[:1])], axis=0)
    summed = jnp.zeros_like(part_rows).at[part_index, rows_low].add(own_term)
    summed = summed.at[part_index, rows_up].add(returned)
    return summed.reshape(-1, R)


def reference(start_factors, bin_factors, tile_speed, tile_weight, tile_cells, tile_count, inner_pairs, inner_weight, face_rows, face_count, face_weight):
    def operator(field):
        summed = tile_image(field, bin_factors, tile_cells, tile_count, tile_weight)
        summed = summed + inner_image(field, inner_pairs, inner_weight)
        summed = summed + face_image(field, face_rows, face_count, face_weight)
        return summed + ridge_weight * field

    rhs_rows = right_side(bin_factors, tile_speed, tile_weight, tile_cells, tile_count)
    solution = start_factors
    residual = rhs_rows - operator(start_factors)
    direction = residual
    norm_now = jnp.sum(residual * residual)
    for iteration in range(ITERS):
        images = operator(direction)
        step_size = norm_now / jnp.sum(direction * images)
        solution = solution + step_size * direction
        residual = residual - step_size * images
        norm_next = jnp.sum(residual * residual)
        direction = residual + (norm_next / norm_now) * direction
        norm_now = norm_next
    return solution, residual
```

```python
import jax
import jax.numpy as jnp
from jax import lax
from jax.sharding import PartitionSpec as P

ITERS = 2
PAD = 8

highest = lax.Precision.HIGHEST
ridge_weight = 0.5


def is_power_of_two(n):
    return n & (n - 1) == 0


def swap(x, axis, mask):
    n = lax.axis_size(axis)
    return lax.ppermute(x, axis, [(i, i ^ mask) for i in range(n)])


def bit_of(axis, mask):
    return (lax.axis_index(axis) & mask) != 0


def ordered(bit, mine, other, dim):
    first = jnp.where(bit, other, mine)
    second = jnp.where(bit, mine, other)
    return jnp.stack([first, second], dim)


def gather_rows(own):
    n = lax.axis_size("bin")
    if not is_power_of_two(n):
        return lax.all_gather(own, "bin", axis=0, tiled=True)
    held = own[None]
    mask = n // 2
    while mask:
        held = ordered(bit_of("bin", mask), held, swap(held, "bin", mask), 1)
        held = held.reshape((-1,) + own.shape)
        mask //= 2
    return held.reshape(-1, own.shape[-1])


def reduce_all(partial_rows):
    n = lax.axis_size("bin")
    if n == 1:
        return partial_rows
    if not is_power_of_two(n):
        return lax.psum(partial_rows, "bin")
    half = partial_rows.shape[0] // 2
    odd = bit_of("bin", 1)
    low, high = partial_rows[:half], partial_rows[half:]
    kept = jnp.where(odd, high, low) + swap(jnp.where(odd, low, high), "bin", 1)
    mask = 2
    while mask < n:
        kept = kept + swap(kept, "bin", mask)
        mask *= 2
    return ordered(odd, kept, swap(kept, "bin", 1), 0).reshape(partial_rows.shape)


def reduce_own(partial_rows, sums):
    n = lax.axis_size("bin")
    width = partial_rows.shape[1]
    if not is_power_of_two(n):
        own = lax.psum_scatter(partial_rows, "bin", scatter_dimension=0, tiled=True)
        return own, lax.psum(sums, "bin")
    blocks = partial_rows.reshape(n, -1, width)
    mask = 1
    while mask < n:
        split = blocks.reshape(-1, 2, blocks.shape[1], width)
        bit = bit_of("bin", mask)
        sent = jnp.where(bit, split[:, 0], split[:, 1])
        kept = jnp.where(bit, split[:, 1], split[:, 0])
        count = sent.shape[0] * sent.shape[1]
        message = jnp.concatenate([sent.reshape(count, width), sums], 0)
        got = swap(message, "bin", mask)
        blocks = kept + got[:count].reshape(kept.shape)
        sums = sums + got[count:]
        mask *= 2
    return blocks.reshape(-1, width), sums


def reduce_seg(sums):
    n = lax.axis_size("seg")
    if not is_power_of_two(n):
        return lax.psum(sums, "seg")
    mask = 1
    while mask < n:
        if mask * 2 < n:
            sums = sums + swap(sums, "seg", mask) + swap(sums, "seg", 2 * mask) + swap(sums, "seg", 3 * mask)
            mask *= 4
        else:
            sums = sums + swap(sums, "seg", mask)
            mask *= 2
    return sums


def pack(values, width):
    rows = [jnp.full((1, width), value, jnp.float32) for value in values]
    rows.append(jnp.zeros((PAD - len(values), width), jnp.float32))
    return jnp.concatenate(rows, 0)


def exchange_faces(low, up):
    n = lax.axis_size("seg")
    odd = bit_of("seg", 1)
    pairs_even = [(i, i + 1) for i in range(0, n - 1, 2)]
    pairs_odd = [(i, i + 1) for i in range(1, n - 1, 2)]
    both = lambda pairs: pairs + [(b, a) for a, b in pairs]
    first = lax.ppermute(jnp.where(odd, low, up), "seg", both(pairs_even))
    second = lax.ppermute(jnp.where(odd, up, low), "seg", both(pairs_odd))
    return jnp.where(odd, first, second), jnp.where(odd, second, first)


def shards(
    start_factors,
    bin_factors,
    tile_speed,
    tile_weight,
    tile_cells,
    tile_count,
    inner_pairs,
    inner_weight,
    face_rows,
    face_count,
    face_weight,
):
    speeds = tile_speed[0, 0]
    weights = tile_weight[0, 0]
    cells = tile_cells[0, 0]
    n_tiles = speeds.shape[0]
    tile_size = speeds.shape[1]
    own_rows = start_factors.shape[0]
    width = start_factors.shape[1]
    n_bin = lax.axis_size("bin")
    n_seg = lax.axis_size("seg")
    part_rows = own_rows * n_bin
    part_blocks = part_rows // tile_size

    start_whole = gather_rows(start_factors)

    rows_low = face_rows[0, 0, 0]
    rows_up = face_rows[0, 0, 1]
    faces = rows_low.shape[0]
    face_slots = jnp.arange(faces, dtype=jnp.int32)
    mask_low = (face_slots < face_count[0, 0, 0]).astype(jnp.float32)
    mask_up = (face_slots < face_count[0, 0, 1]).astype(jnp.float32)
    count_up = face_count[0, 0, 1].astype(jnp.float32)
    block_low = face_weight[0, 0] * mask_low[:, None]
    block_next = lax.ppermute(block_low, "seg", [(i, i - 1) for i in range(1, n_seg)])

    block_ids = jnp.arange(part_blocks, dtype=jnp.int32)
    live_tiles = (jnp.arange(n_tiles, dtype=jnp.int32) < tile_count[0, 0]).astype(jnp.float32)
    tile_bins = bin_factors.reshape(-1, tile_size, width)[cells[:, 1]]
    bins_wide = tile_bins.astype(jnp.float32)
    tile_gain = weights.astype(jnp.float32) * live_tiles[:, None, None]
    tile_onehot = (cells[:, 0][:, None] == block_ids[None, :]).astype(jnp.float32)
    weighted = (weights.astype(jnp.float32) * speeds.astype(jnp.float32)).astype(jnp.bfloat16)
    rhs_terms = jnp.einsum("kij,kjr->kir", weighted, tile_bins, preferred_element_type=jnp.float32)
    rhs_terms = rhs_terms * live_tiles[:, None, None]
    rhs_part = jnp.einsum("kb,kir->bir", tile_onehot, rhs_terms, precision=highest).reshape(
        part_rows, width
    )
    pairs = inner_pairs[0, 0]
    pair_weight = inner_weight[0, 0]
    left_onehot = (pairs[:, 0][:, None] == block_ids[None, :]).astype(jnp.float32)
    right_onehot = (pairs[:, 1][:, None] == block_ids[None, :]).astype(jnp.float32)
    left_degree = pair_weight.sum(2)
    right_degree = pair_weight.sum(1)

    coupling = []

    def apply_local(whole_rows, extra):
        own_low = whole_rows[rows_low] * mask_low[:, None]
        own_up = whole_rows[rows_up] * mask_up[:, None]
        low_message = jnp.concatenate([own_low, extra], 0)
        up_message = jnp.concatenate([own_up, extra], 0)
        up_previous, low_next = exchange_faces(low_message, up_message)

        blocks = whole_rows.reshape(part_blocks, tile_size, width)
        picked = blocks[cells[:, 0]]
        scores = jnp.einsum("kir,kjr->kij", picked, bins_wide, precision=highest) * tile_gain
        pulled = jnp.einsum("kij,kjr->kir", scores, bins_wide, precision=highest)
        left = blocks[pairs[:, 0]]
        right = blocks[pairs[:, 1]]
        to_left = left_degree[..., None] * left - jnp.einsum(
            "kij,kjr->kir", pair_weight, right, precision=highest
        )
        to_right = right_degree[..., None] * right - jnp.einsum(
            "kij,kir->kjr", pair_weight, left, precision=highest
        )
        summed = jnp.einsum("kb,kir->bir", tile_onehot, pulled, precision=highest)
        summed = summed + jnp.einsum("kb,kir->bir", left_onehot, to_left, precision=highest)
        summed = summed + jnp.einsum("kb,kir->bir", right_onehot, to_right, precision=highest)
        summed = summed.reshape(part_rows, width)

        if not coupling:
            live_previous = (face_slots.astype(jnp.float32) < up_previous[faces, 0]).astype(jnp.float32)
            coupling.append(block_low * live_previous[None, :])
            coupling.append(block_next * mask_up[None, :])
        down, up = coupling
        low_term = down.sum(1)[:, None] * own_low - jnp.dot(
            down, up_previous[:faces], precision=highest
        )
        up_term = up.sum(0)[:, None] * own_up - jnp.dot(
            up.T, low_next[:faces], precision=highest
        )
        return summed.at[rows_low].add(low_term).at[rows_up].add(up_term)

    counts = pack([count_up], width)
    partial_zero = rhs_part - apply_local(start_whole, counts)
    first = reduce_all(partial_zero) - ridge_weight * start_whole
    second = reduce_all(apply_local(first, counts)) + ridge_weight * first
    early = reduce_seg(pack([jnp.sum(first * first), jnp.sum(first * second)], width))
    norm_zero, product_zero = early[0, 0], early[1, 0]
    step_zero = norm_zero / product_zero
    partial_two = apply_local(second, counts)
    residual_whole = first - step_zero * second
    late_part = pack([jnp.sum(residual_whole * partial_two)], width)
    third, late = reduce_own(partial_two, late_part)
    with_second = jnp.sum(residual_whole * second)
    product_part = with_second - step_zero * (late[0, 0] + ridge_weight * with_second)
    final = reduce_seg(pack([jnp.sum(residual_whole * residual_whole), product_part], width))
    norm_one, product_one = final[0, 0], final[1, 0]
    beta = norm_one / norm_zero
    step_one = norm_one / (product_one - beta * norm_one / step_zero)

    offset = lax.axis_index("bin") * own_rows
    own = lambda whole: lax.dynamic_slice(whole, (offset, 0), (own_rows, width))
    first, second = own(first), own(second)
    third = third + ridge_weight * second
    residual = first - step_zero * second
    image = second - step_zero * third
    direction = residual + beta * first
    along = image + beta * second
    solution_factors = start_factors + step_zero * first + step_one * direction
    residual = residual - step_one * along
    return solution_factors, residual


def solution(mesh):
    return jax.shard_map(
        shards,
        mesh=mesh,
        in_specs=(
            P(("groups", "seg", "bin"), None),
            P(("groups", "bin"), None),
            P(("groups", "seg"), "bin", None, None, None),
            P(("groups", "seg"), "bin", None, None, None),
            P(("groups", "seg"), "bin", None, None),
            P(("groups", "seg"), "bin"),
            P(("groups", "seg"), "bin", None, None),
            P(("groups", "seg"), "bin", None, None, None),
            P(("groups", "seg"), "bin", None, None),
            P(("groups", "seg"), "bin", None),
            P(("groups", "seg"), "bin", None, None),
        ),
        out_specs=(P(("groups", "seg", "bin"), None), P(("groups", "seg", "bin"), None)),
        check_vma=False,
    )
```

```python
import functools

import jax
import jax.numpy as jnp
from jax import lax
from jax.experimental import pallas as pl
from jax.experimental.pallas import tpu as pltpu
from jax.sharding import PartitionSpec as P

ITERS = 2
PAD = 8
VMEM_BYTES = 16 << 20

f32 = jnp.float32
bf16 = jnp.bfloat16
ridge_weight = 0.5


def is_power_of_two(n):
    return n & (n - 1) == 0


def swap(x, axis, mask):
    n = lax.axis_size(axis)
    return lax.ppermute(x, axis, [(i, i ^ mask) for i in range(n)])


def bit_of(axis, mask):
    return (lax.axis_index(axis) & mask) != 0


def ordered(bit, mine, other, dim):
    first = jnp.where(bit, other, mine)
    second = jnp.where(bit, mine, other)
    return jnp.stack([first, second], dim)


def gather_rows(own):
    n = lax.axis_size("bin")
    if not is_power_of_two(n):
        return lax.all_gather(own, "bin", axis=0, tiled=True)
    held = own[None]
    mask = n // 2
    while mask:
        held = ordered(bit_of("bin", mask), held, swap(held, "bin", mask), 1)
        held = held.reshape((-1,) + own.shape)
        mask //= 2
    return held.reshape(-1, own.shape[-1])


def reduce_all(partial_rows):
    n = lax.axis_size("bin")
    if n == 1:
        return partial_rows
    if not is_power_of_two(n):
        return lax.psum(partial_rows, "bin")
    half = partial_rows.shape[0] // 2
    odd = bit_of("bin", 1)
    low, high = partial_rows[:half], partial_rows[half:]
    kept = jnp.where(odd, high, low) + swap(jnp.where(odd, low, high), "bin", 1)
    mask = 2
    while mask < n:
        kept = kept + swap(kept, "bin", mask)
        mask *= 2
    return ordered(odd, kept, swap(kept, "bin", 1), 0).reshape(partial_rows.shape)


def reduce_own(partial_rows, sums):
    n = lax.axis_size("bin")
    width = partial_rows.shape[1]
    if not is_power_of_two(n):
        own = lax.psum_scatter(partial_rows, "bin", scatter_dimension=0, tiled=True)
        return own, lax.psum(sums, "bin")
    blocks = partial_rows.reshape(n, -1, width)
    mask = 1
    while mask < n:
        split = blocks.reshape(-1, 2, blocks.shape[1], width)
        bit = bit_of("bin", mask)
        sent = jnp.where(bit, split[:, 0], split[:, 1])
        kept = jnp.where(bit, split[:, 1], split[:, 0])
        count = sent.shape[0] * sent.shape[1]
        message = jnp.concatenate([sent.reshape(count, width), sums], 0)
        got = swap(message, "bin", mask)
        blocks = kept + got[:count].reshape(kept.shape)
        sums = sums + got[count:]
        mask *= 2
    return blocks.reshape(-1, width), sums


def reduce_seg(sums):
    n = lax.axis_size("seg")
    if not is_power_of_two(n):
        return lax.psum(sums, "seg")
    mask = 1
    while mask < n:
        if mask * 2 < n:
            sums = sums + swap(sums, "seg", mask) + swap(sums, "seg", 2 * mask) + swap(sums, "seg", 3 * mask)
            mask *= 4
        else:
            sums = sums + swap(sums, "seg", mask)
            mask *= 2
    return sums


def exchange_pairs(n, first):
    pairs = [(i, i + 1) for i in range(first, n - 1, 2)]
    return pairs + [(b, a) for a, b in pairs]


def exchange_faces(message_even, message_odd):
    n = lax.axis_size("seg")
    got_even = lax.ppermute(message_even, "seg", exchange_pairs(n, 0))
    got_odd = lax.ppermute(message_odd, "seg", exchange_pairs(n, 1))
    return got_even, got_odd


def split(x):
    high = x.astype(bf16)
    return high, (x - high.astype(f32)).astype(bf16)


def dot(a, b):
    return lax.dot_general(a, b, (((1,), (0,)), ((), ())), preferred_element_type=f32)


def along(x):
    high, low = split(x)
    return jnp.concatenate([high, high, low], 1)


def stacked(x):
    high, low = split(x)
    return jnp.concatenate([high, low, high], 0)


class Info:
    def __init__(self, n_tiles, n_inner):
        self.cells = 0
        self.count = 2 * n_tiles
        self.pairs = self.count + 1
        self.faces = self.pairs + 2 * n_inner
        self.odd = self.faces + 2
        self.index = self.odd + 1


def call(kernel, outs, *operands, scratch=(), flops=0):
    smem = pl.BlockSpec(memory_space=pltpu.SMEM)
    vmem = pl.BlockSpec(memory_space=pltpu.VMEM)
    nbytes = sum(o.size * o.dtype.itemsize for o in operands)
    return pl.pallas_call(
        kernel,
        out_shape=[jax.ShapeDtypeStruct(shape, kind) for shape, kind in outs],
        in_specs=[smem] + [vmem] * (len(operands) - 1),
        out_specs=[vmem] * len(outs),
        scratch_shapes=scratch,
        compiler_params=pltpu.CompilerParams(vmem_limit_bytes=VMEM_BYTES),
        cost_estimate=pl.CostEstimate(flops=flops, bytes_accessed=nbytes, transcendentals=0),
    )(*operands)


def prep_kernel(at, n_bin, info, weights, speeds, bins, inner, rows, face,
                rhs, gain, bins_t, bins_s, inner_cat, diag, pick_hot, scatter_hot, down_cat):
    n_tiles, tile, _ = weights.shape
    width = bins.shape[1]
    part_rows = rhs.shape[0]
    for k in range(bins.shape[0] // tile):
        block = bins[k * tile:(k + 1) * tile, :]
        flipped = block.astype(f32).T.astype(bf16)
        bins_t[k] = jnp.concatenate([flipped, flipped], 0)
        bins_s[k] = jnp.concatenate([block, block], 0)
    rhs[...] = jnp.zeros_like(rhs)
    for k in range(n_tiles):
        wide = weights[k].astype(f32)
        live = jnp.where(k < info[at.count], 1.0, 0.0).astype(f32)
        gain[k] = wide * live
        weighted = (wide * speeds[k].astype(f32)).astype(bf16)
        terms = dot(weighted, bins_s[info[at.cells + 2 * k + 1], 0:tile, :]) * live
        place = pl.ds(pl.multiple_of(info[at.cells + 2 * k] * tile, tile), tile)
        rhs[place, :] += terms
    diag[...] = jnp.full(diag.shape, ridge_weight / n_bin, f32)
    for j in range(inner.shape[0]):
        block = inner[j]
        flipped = block.T
        inner_cat[j, 0] = along(block)
        inner_cat[j, 1] = along(flipped)
        for side, matrix in enumerate((block, flipped)):
            place = pl.ds(pl.multiple_of(info[at.pairs + 2 * j + side] * tile, tile), tile)
            degree = jnp.sum(matrix, axis=1, keepdims=True)
            diag[place, :] += jnp.broadcast_to(degree, (tile, width))
    n_face = rows.shape[1]
    for side in range(2):
        live = info[at.faces + side]
        listed = rows[side:side + 1, :]
        slots = lax.broadcasted_iota(jnp.int32, (1, n_face), 1)
        listed = jnp.where(slots < live, listed, -1)
        ids = lax.broadcasted_iota(jnp.int32, (part_rows, n_face), 0)
        hot = (ids == listed).astype(f32)
        scatter_hot[:, side * n_face:(side + 1) * n_face] = hot.astype(bf16)
        pick_hot[side * n_face:(side + 1) * n_face, :] = hot.T.astype(bf16)
    high, low = split(face[...])
    hot = scatter_hot[:, 0:n_face]
    high = dot(hot, high).astype(bf16)
    low = dot(hot, low).astype(bf16)
    down_cat[...] = jnp.concatenate([high, high, low], 1)


def up_kernel(info, face_next, scatter_hot, up_cat):
    n_face = face_next.shape[0]
    high, low = split(face_next[...].T)
    hot = scatter_hot[:, n_face:2 * n_face]
    high = dot(hot, high).astype(bf16)
    low = dot(hot, low).astype(bf16)
    up_cat[...] = jnp.concatenate([high, high, low], 1)


def pick_kernel(at, count_row, info, whole, pick_hot, *refs):
    if count_row:
        whole_cat, even, odd = refs
        extra = jnp.full((PAD, whole.shape[1]), info[at.faces + 1], jnp.int32).astype(f32)
    else:
        before, whole_cat, even, odd, sums = refs
        extra = None
    high, low = split(whole[...])
    cat = jnp.concatenate([high, low], 1)
    whole_cat[...] = cat
    width = whole.shape[1]
    picked = dot(pick_hot[...], cat)
    picked = picked[:, :width] + picked[:, width:]
    n_face = picked.shape[0] // 2
    low_rows, up_rows = picked[:n_face], picked[n_face:]
    is_odd = info[at.odd] == 1
    even[0:n_face, :] = jnp.where(is_odd, low_rows, up_rows)
    odd[0:n_face, :] = jnp.where(is_odd, up_rows, low_rows)
    if count_row:
        even[n_face:, :] = extra
        odd[n_face:, :] = extra
    else:
        now, old = whole[...], before[...]
        sums[...] = jnp.zeros_like(sums)
        sums[0:1, :] = jnp.sum(old * old, axis=0, keepdims=True)
        sums[1:2, :] = jnp.sum(old * now, axis=0, keepdims=True)


def main_kernel(at, info, whole, whole_cat, bins_t, bins_s, gain, inner_cat, diag, out, terms):
    n_tiles, tile, _ = gain.shape
    width = whole.shape[1]
    for k in range(n_tiles):
        place = pl.ds(pl.multiple_of(info[at.cells + 2 * k] * tile, tile), tile)
        column = info[at.cells + 2 * k + 1]
        scores = dot(whole_cat[place, :], bins_t[column]) * gain[k]
        high, low = split(scores)
        terms[k] = dot(jnp.concatenate([high, low], 1), bins_s[column])
    n_inner = inner_cat.shape[0]
    for j in range(n_inner):
        for side in range(2):
            place = pl.ds(pl.multiple_of(info[at.pairs + 2 * j + 1 - side] * tile, tile), tile)
            other = whole_cat[place, :]
            high, low = other[:, :width], other[:, width:]
            terms[n_tiles + 2 * j + side] = -dot(inner_cat[j, side], jnp.concatenate([high, low, high], 0))
    out[...] = diag[...] * whole[...]
    for k in range(n_tiles):
        place = pl.ds(pl.multiple_of(info[at.cells + 2 * k] * tile, tile), tile)
        out[place, :] += terms[k]
    for j in range(n_inner):
        for side in range(2):
            place = pl.ds(pl.multiple_of(info[at.pairs + 2 * j + side] * tile, tile), tile)
            out[place, :] += terms[n_tiles + 2 * j + side]


def neighbours(at, info, even, odd, n_face):
    is_odd = info[at.odd] == 1
    first, second = even[0:n_face, :], odd[0:n_face, :]
    return jnp.where(is_odd, first, second), jnp.where(is_odd, second, first)


def first_face_kernel(at, info, even, odd, down_cat, up_cat, part, whole, diag, rhs, out, diag_all):
    n_face = down_cat.shape[1] // 3
    width = part.shape[1]
    previous, following = neighbours(at, info, even, odd, n_face)
    is_odd = info[at.odd] == 1
    count = jnp.where(is_odd, even[n_face:n_face + 1, :], odd[n_face:n_face + 1, :])
    slots = lax.broadcasted_iota(jnp.int32, (n_face, width), 0).astype(f32)
    live = jnp.where(slots < count, 1.0, 0.0).astype(bf16)
    zero, one = jnp.zeros_like(live), jnp.ones_like(live)
    down = jnp.concatenate([stacked(previous), jnp.concatenate([live, zero, live], 0)], 1)
    up = jnp.concatenate([stacked(following), jnp.concatenate([one, zero, one], 0)], 1)
    both = dot(down_cat[...], down) + dot(up_cat[...], up)
    degree = both[:, width:]
    diag_all[...] = diag[...] + degree
    out[...] = rhs[...] - (part[...] + degree * whole[...] - both[:, :width])


def face_kernel(at, info, even, odd, down_cat, up_cat, part, out):
    n_face = down_cat.shape[1] // 3
    previous, following = neighbours(at, info, even, odd, n_face)
    out[...] = part[...] - dot(down_cat[...], stacked(previous)) - dot(up_cat[...], stacked(following))


def row_sum(values):
    return jnp.sum(values, axis=1, keepdims=True)


def last_face_kernel(at, info, even, odd, down_cat, up_cat, part, first, second, early, out, sums, known):
    n_face = down_cat.shape[1] // 3
    previous, following = neighbours(at, info, even, odd, n_face)
    image = part[...] - dot(down_cat[...], stacked(previous)) - dot(up_cat[...], stacked(following))
    out[...] = image
    step = row_sum(early[0:1, :]) / row_sum(early[1:2, :])
    residual = first[...] - step * second[...]
    sums[...] = jnp.zeros_like(sums)
    sums[0:1, :] = jnp.sum(residual * image, axis=0, keepdims=True)
    known[...] = jnp.zeros_like(known)
    known[0:1, :] = jnp.sum(residual * residual, axis=0, keepdims=True)
    known[1:2, :] = jnp.sum(residual * second[...], axis=0, keepdims=True)


def step_kernel(info, early, known, late, out):
    step = row_sum(early[0:1, :]) / row_sum(early[1:2, :])
    out[...] = jnp.zeros_like(out)
    out[0:1, :] = known[0:1, :]
    out[1:2, :] = known[1:2, :] - step * late[0:1, :]


def last_kernel(at, info, start, first, second, third, early, final, solution, residual):
    own_rows = start.shape[0]
    place = pl.ds(pl.multiple_of(info[at.index] * own_rows, own_rows), own_rows)
    norm_zero, product_zero = row_sum(early[0:1, :]), row_sum(early[1:2, :])
    norm_one, product_one = row_sum(final[0:1, :]), row_sum(final[1:2, :])
    step_zero = norm_zero / product_zero
    beta = norm_one / norm_zero
    step_one = norm_one / (product_one - beta * norm_one / step_zero)
    zeroth, once, twice = first[place, :], second[place, :], third[...]
    after = zeroth - step_zero * once
    image = once - step_zero * twice
    direction = after + beta * zeroth
    moved = image + beta * once
    solution[...] = start[...] + step_zero * zeroth + step_one * direction
    residual[...] = after - step_one * moved


def shards(
    start_factors,
    bin_factors,
    tile_speed,
    tile_weight,
    tile_cells,
    tile_count,
    inner_pairs,
    inner_weight,
    face_rows,
    face_count,
    face_weight,
):
    start_whole = gather_rows(start_factors)
    weights = tile_weight[0, 0]
    n_tiles, tile, _ = weights.shape
    inner = inner_weight[0, 0]
    n_inner = inner.shape[0]
    rows = face_rows[0, 0]
    n_face = rows.shape[1]
    own_rows, width = start_factors.shape
    n_bin = lax.axis_size("bin")
    n_seg = lax.axis_size("seg")
    part_rows = own_rows * n_bin
    bin_blocks = bin_factors.shape[0] // tile
    at = Info(n_tiles, n_inner)
    info = jnp.concatenate(
        [
            tile_cells.reshape(-1),
            tile_count.reshape(-1),
            inner_pairs.reshape(-1),
            face_count.reshape(-1),
            (lax.axis_index("seg") % 2).reshape(1),
            lax.axis_index("bin").reshape(1),
        ]
    ).astype(jnp.int32)

    face = face_weight[0, 0]
    live_low = (jnp.arange(n_face, dtype=jnp.int32) < face_count[0, 0, 0]).astype(f32)
    face_next = lax.ppermute(
        face * live_low[:, None], "seg", [(i, i - 1) for i in range(1, n_seg)]
    )

    rows_shape = (part_rows, width)
    tile_flops = 2 * tile * tile * width
    rhs, gain, bins_t, bins_s, inner_cat, diag, pick_hot, scatter_hot, down_cat = call(
        functools.partial(prep_kernel, at, n_bin),
        [
            (rows_shape, f32),
            ((n_tiles, tile, tile), f32),
            ((bin_blocks, 2 * width, tile), bf16),
            ((bin_blocks, 2 * tile, width), bf16),
            ((n_inner, 2, tile, 3 * tile), bf16),
            (rows_shape, f32),
            ((2 * n_face, part_rows), bf16),
            ((part_rows, 2 * n_face), bf16),
            ((part_rows, 3 * n_face), bf16),
        ],
        info,
        weights,
        tile_speed[0, 0],
        bin_factors,
        inner,
        rows,
        face,
        flops=n_tiles * tile_flops,
    )
    (up_cat,) = call(
        up_kernel, [((part_rows, 3 * n_face), bf16)], info, face_next, scatter_hot, flops=tile_flops
    )

    message = ((n_face + PAD, width), f32)
    cat = ((part_rows, 2 * width), bf16)
    sums = ((PAD, width), f32)

    def main(whole, whole_cat, diagonal):
        (part,) = call(
            functools.partial(main_kernel, at),
            [(rows_shape, f32)],
            info,
            whole,
            whole_cat,
            bins_t,
            bins_s,
            gain,
            inner_cat,
            diagonal,
            scratch=[pltpu.VMEM((n_tiles + 2 * n_inner, tile, width), f32)],
            flops=6 * n_tiles * tile_flops,
        )
        return part

    start_cat, even, odd = call(
        functools.partial(pick_kernel, at, True), [cat, message, message], info, start_whole, pick_hot
    )
    even, odd = exchange_faces(even, odd)
    part = main(start_whole, start_cat, diag)
    part, diag_all = call(
        functools.partial(first_face_kernel, at),
        [(rows_shape, f32), (rows_shape, f32)],
        info, even, odd, down_cat, up_cat, part, start_whole, diag, rhs,
    )
    first = reduce_all(part)

    first_cat, even, odd = call(
        functools.partial(pick_kernel, at, True), [cat, message, message], info, first, pick_hot
    )
    even, odd = exchange_faces(even, odd)
    part = main(first, first_cat, diag_all)
    (part,) = call(
        functools.partial(face_kernel, at), [(rows_shape, f32)], info, even, odd, down_cat, up_cat, part
    )
    second = reduce_all(part)

    face_message = ((n_face, width), f32)
    second_cat, even, odd, early = call(
        functools.partial(pick_kernel, at, False),
        [cat, face_message, face_message, sums], info, second, pick_hot, first,
    )
    even, odd = exchange_faces(even, odd)
    early = reduce_seg(early)
    part = main(second, second_cat, diag_all)
    part, late, known = call(
        functools.partial(last_face_kernel, at),
        [(rows_shape, f32), sums, sums],
        info, even, odd, down_cat, up_cat, part, first, second, early,
    )
    third, late = reduce_own(part, late)
    (final,) = call(step_kernel, [sums], info, early, known, late)
    final = reduce_seg(final)
    return tuple(
        call(
            functools.partial(last_kernel, at),
            [(start_factors.shape, f32), (start_factors.shape, f32)],
            info, start_factors, first, second, third, early, final,
        )
    )


def solution(mesh):
    return jax.shard_map(
        shards,
        mesh=mesh,
        in_specs=(
            P(("groups", "seg", "bin"), None),
            P(("groups", "bin"), None),
            P(("groups", "seg"), "bin", None, None, None),
            P(("groups", "seg"), "bin", None, None, None),
            P(("groups", "seg"), "bin", None, None),
            P(("groups", "seg"), "bin"),
            P(("groups", "seg"), "bin", None, None),
            P(("groups", "seg"), "bin", None, None, None),
            P(("groups", "seg"), "bin", None, None),
            P(("groups", "seg"), "bin", None),
            P(("groups", "seg"), "bin", None, None),
        ),
        out_specs=(P(("groups", "seg", "bin"), None), P(("groups", "seg", "bin"), None)),
        check_vma=False,
    )
```

```python
import functools

import jax
import jax.numpy as jnp
from jax import lax
from jax.experimental import pallas as pl
from jax.experimental.pallas import tpu as pltpu
from jax.sharding import PartitionSpec as P

ITERS = 2
PAD = 8
VMEM_BYTES = 16 << 20

f32 = jnp.float32
bf16 = jnp.bfloat16
ridge_weight = 0.5


def is_power_of_two(n):
    return n & (n - 1) == 0


def swap(x, axis, mask):
    n = lax.axis_size(axis)
    return lax.ppermute(x, axis, [(i, i ^ mask) for i in range(n)])


def bit_of(axis, mask):
    return (lax.axis_index(axis) & mask) != 0


def ordered(bit, mine, other, dim):
    first = jnp.where(bit, other, mine)
    second = jnp.where(bit, mine, other)
    return jnp.stack([first, second], dim)


def gather_rows(own, copy):
    n = lax.axis_size("bin")
    if not is_power_of_two(n):
        return lax.all_gather(own, "bin", axis=0, tiled=True)
    sent, held = own[None], copy[None]
    mask = n // 2
    while mask:
        held = ordered(bit_of("bin", mask), held, swap(sent, "bin", mask), 1)
        held = held.reshape((-1,) + own.shape)
        sent = held
        mask //= 2
    return held.reshape(-1, own.shape[-1])


def reduce_all(partial_rows):
    n = lax.axis_size("bin")
    if n == 1:
        return partial_rows
    if not is_power_of_two(n):
        return lax.psum(partial_rows, "bin")
    half = partial_rows.shape[0] // 2
    odd = bit_of("bin", 1)
    low, high = partial_rows[:half], partial_rows[half:]
    kept = jnp.where(odd, high, low) + swap(jnp.where(odd, low, high), "bin", 1)
    mask = 2
    while mask < n:
        kept = kept + swap(kept, "bin", mask)
        mask *= 2
    return ordered(odd, kept, swap(kept, "bin", 1), 0).reshape(partial_rows.shape)


def reduce_own(partial_rows, sums):
    n = lax.axis_size("bin")
    width = partial_rows.shape[1]
    if not is_power_of_two(n):
        own = lax.psum_scatter(partial_rows, "bin", scatter_dimension=0, tiled=True)
        return own, lax.psum(sums, "bin")
    blocks = partial_rows.reshape(n, -1, width)
    mask = 1
    while mask < n:
        split = blocks.reshape(-1, 2, blocks.shape[1], width)
        bit = bit_of("bin", mask)
        sent = jnp.where(bit, split[:, 0], split[:, 1])
        kept = jnp.where(bit, split[:, 1], split[:, 0])
        count = sent.shape[0] * sent.shape[1]
        message = jnp.concatenate([sent.reshape(count, width), sums], 0)
        got = swap(message, "bin", mask)
        blocks = kept + got[:count].reshape(kept.shape)
        sums = sums + got[count:]
        mask *= 2
    return blocks.reshape(-1, width), sums


def reduce_seg(sums):
    n = lax.axis_size("seg")
    if not is_power_of_two(n):
        return lax.psum(sums, "seg")
    mask = 1
    while mask < n:
        if mask * 2 < n:
            sums = sums + swap(sums, "seg", mask) + swap(sums, "seg", 2 * mask) + swap(sums, "seg", 3 * mask)
            mask *= 4
        else:
            sums = sums + swap(sums, "seg", mask)
            mask *= 2
    return sums


def face_pairs(first):
    n_seg, n_bin = lax.axis_size("seg"), lax.axis_size("bin")
    pairs = []
    for s in range(n_seg):
        other = s + 1 if (s - first) % 2 == 0 else s - 1
        for t in range(n_bin):
            if 0 <= other < n_seg:
                pairs.append((s * n_bin + t, other * n_bin + t))
            elif n_bin % 2 == 0:
                pairs.append((s * n_bin + t, s * n_bin + (t ^ 1)))
    return pairs


def exchange_faces(message_even, message_odd):
    got_even = lax.ppermute(message_even, ("seg", "bin"), face_pairs(0))
    got_odd = lax.ppermute(message_odd, ("seg", "bin"), face_pairs(1))
    return got_even, got_odd


def split(x):
    high = x.astype(bf16)
    return high, (x - high.astype(f32)).astype(bf16)


def dot(a, b):
    return lax.dot_general(a, b, (((1,), (0,)), ((), ())), preferred_element_type=f32)


def along(x):
    high, low = split(x)
    return jnp.concatenate([high, high, low], 1)


def stacked(x):
    high, low = split(x)
    return jnp.concatenate([high, low, high], 0)


def call(kernel, outs, *operands, smem=(), hbm=False, scratch=(), flops=0):
    in_smem = pl.BlockSpec(memory_space=pltpu.SMEM)
    in_vmem = pl.BlockSpec(memory_space=pltpu.VMEM)
    given = pl.BlockSpec(memory_space=pltpu.HBM) if hbm else in_vmem
    nbytes = sum(o.size * o.dtype.itemsize for o in operands)
    return pl.pallas_call(
        kernel,
        out_shape=[jax.ShapeDtypeStruct(shape, kind) for shape, kind in outs],
        in_specs=[in_smem] * len(smem) + [given] * len(operands),
        out_specs=[in_vmem] * len(outs),
        scratch_shapes=scratch,
        compiler_params=pltpu.CompilerParams(vmem_limit_bytes=VMEM_BYTES),
        cost_estimate=pl.CostEstimate(flops=flops, bytes_accessed=nbytes, transcendentals=0),
    )(*smem, *operands)


def block_at(index, size):
    return pl.ds(pl.multiple_of(index * size, size), size)


def prep_kernel(n_bin, cells, count, pairs, faces,
                start_hbm, bins_hbm, rows_hbm, face_hbm, inner_hbm, weights_hbm, speeds_hbm,
                start, rhs, gain, bins_t, bins_s, inner_cat, diag, pick_hot, scatter_up, down_cat,
                bins, rows, face, inner, weights, speeds, sems):
    moves = [
        pltpu.make_async_copy(source, target, sems.at[i])
        for i, (source, target) in enumerate([
            (rows_hbm, rows), (face_hbm, face), (start_hbm, start), (bins_hbm, bins),
            (inner_hbm, inner), (weights_hbm, weights), (speeds_hbm, speeds),
        ])
    ]
    for move in moves:
        move.start()
    n_tiles, tile, _ = weights.shape
    width = bins.shape[1]
    part_rows = rhs.shape[0]
    n_face = rows.shape[1]
    is_odd = lax.axis_index("seg") % 2 == 1
    is_first = lax.axis_index("seg") == 0
    rhs[...] = jnp.zeros_like(rhs)
    diag[...] = jnp.full(diag.shape, ridge_weight / n_bin, f32)
    slots = lax.broadcasted_iota(jnp.int32, (1, n_face), 1)
    ids = lax.broadcasted_iota(jnp.int32, (part_rows, n_face), 0)
    moves[0].wait()
    hots = []
    for side in range(2):
        listed = jnp.where(slots < faces[0, side], rows[side:side + 1, :], -1)
        hots.append((ids == listed).astype(f32))
    scatter_up[...] = hots[1].astype(bf16)
    low_t, up_t = hots[0].T.astype(bf16), hots[1].T.astype(bf16)
    pick_hot[0:n_face, :] = jnp.where(is_odd, low_t, up_t)
    pick_hot[n_face:, :] = jnp.where(is_odd, up_t, low_t)
    moves[1].wait()
    high, low = split(jnp.where(is_first, 0.0, face[...]))
    hot = hots[0].astype(bf16)
    high = dot(hot, high).astype(bf16)
    low = dot(hot, low).astype(bf16)
    down_cat[...] = jnp.concatenate([high, high, low], 1)
    moves[2].wait()
    moves[3].wait()
    for k in range(bins.shape[0] // tile):
        block = bins[k * tile:(k + 1) * tile, :]
        flipped = block.astype(f32).T.astype(bf16)
        bins_t[k] = jnp.concatenate([flipped, flipped], 0)
        bins_s[k] = jnp.concatenate([block, block], 0)
    moves[4].wait()
    for j in range(inner.shape[0]):
        block = inner[j]
        flipped = block.T
        inner_cat[j, 0] = along(block)
        inner_cat[j, 1] = along(flipped)
        for side, matrix in enumerate((block, flipped)):
            degree = jnp.sum(matrix, axis=1, keepdims=True)
            diag[block_at(pairs[j, side], tile), :] += jnp.broadcast_to(degree, (tile, width))
    moves[5].wait()
    moves[6].wait()
    for k in range(n_tiles):
        wide = weights[k].astype(f32)
        live = jnp.where(k < count[0, 0], 1.0, 0.0).astype(f32)
        gain[k] = wide * live
        weighted = (wide * speeds[k].astype(f32)).astype(bf16)
        terms = dot(weighted, bins[block_at(cells[1, k], tile), :]) * live
        rhs[block_at(cells[0, k], tile), :] += terms


def up_kernel(face_even, face_odd, scatter_up, down_cat, cat_even, cat_odd):
    index = lax.axis_index("seg")
    is_odd = index % 2 == 1
    is_last = index == lax.axis_size("seg") - 1
    following = jnp.where(is_odd, face_odd[...], face_even[...])
    high, low = split(jnp.where(is_last, 0.0, following).T)
    hot = scatter_up[...]
    high = dot(hot, high).astype(bf16)
    low = dot(hot, low).astype(bf16)
    up = jnp.concatenate([high, high, low], 1)
    down = down_cat[...]
    cat_even[...] = jnp.where(is_odd, down, up)
    cat_odd[...] = jnp.where(is_odd, up, down)


def pick(whole, pick_hot, whole_cat):
    width = whole.shape[1]
    high, low = split(whole[...])
    cat = jnp.concatenate([high, low], 1)
    whole_cat[...] = cat
    picked = dot(pick_hot[...], cat)
    return picked[:, :width] + picked[:, width:]


def first_pick_kernel(whole, pick_hot, counts, whole_cat, even, odd):
    picked = pick(whole, pick_hot, whole_cat)
    n_face = picked.shape[0] // 2
    even[0:n_face, :] = picked[:n_face]
    odd[0:n_face, :] = picked[n_face:]
    even[n_face:, :] = counts[0:PAD, :]
    odd[n_face:, :] = counts[PAD:, :]


def pick_kernel(whole, pick_hot, whole_cat, even, odd):
    picked = pick(whole, pick_hot, whole_cat)
    n_face = picked.shape[0] // 2
    even[...] = picked[:n_face]
    odd[...] = picked[n_face:]


def main_kernel(cells, pairs, whole, whole_cat, bins_t, bins_s, gain, inner_cat, diag, *refs):
    if len(refs) == 4:
        before, out, sums, terms = refs
        now, old = whole[...], before[...]
        sums[...] = jnp.zeros_like(sums)
        sums[0:1, :] = jnp.sum(old * old, axis=0, keepdims=True)
        sums[1:2, :] = jnp.sum(old * now, axis=0, keepdims=True)
    else:
        out, terms = refs
    n_tiles, tile, _ = gain.shape
    width = whole.shape[1]
    for k in range(n_tiles):
        scores = dot(whole_cat[block_at(cells[0, k], tile), :], bins_t[cells[1, k]]) * gain[k]
        high, low = split(scores)
        terms[k] = dot(jnp.concatenate([high, low], 1), bins_s[cells[1, k]])
    n_inner = inner_cat.shape[0]
    for j in range(n_inner):
        for side in range(2):
            other = whole_cat[block_at(pairs[j, 1 - side], tile), :]
            high, low = other[:, :width], other[:, width:]
            terms[n_tiles + 2 * j + side] = -dot(inner_cat[j, side], jnp.concatenate([high, low, high], 0))
    out[...] = diag[...] * whole[...]
    for k in range(n_tiles):
        out[block_at(cells[0, k], tile), :] += terms[k]
    for j in range(n_inner):
        for side in range(2):
            out[block_at(pairs[j, side], tile), :] += terms[n_tiles + 2 * j + side]


def first_face_kernel(even, odd, cat_even, cat_odd, part, whole, diag, rhs, out, diag_all):
    n_face = cat_even.shape[1] // 3
    width = part.shape[1]
    slots = lax.broadcasted_iota(jnp.int32, (n_face, width), 0).astype(f32)
    both = jnp.zeros((part.shape[0], 2 * width), f32)
    for got, cat in ((even, cat_even), (odd, cat_odd)):
        live = jnp.where(slots < got[n_face:n_face + 1, :], 1.0, 0.0).astype(bf16)
        seen = jnp.concatenate([live, jnp.zeros_like(live), live], 0)
        both = both + dot(cat[...], jnp.concatenate([stacked(got[0:n_face, :]), seen], 1))
    degree = both[:, width:]
    diag_all[...] = diag[...] + degree
    out[...] = rhs[...] - (part[...] + degree * whole[...] - both[:, :width])


def face_image(even, odd, cat_even, cat_odd, part):
    return part[...] - dot(cat_even[...], stacked(even[...])) - dot(cat_odd[...], stacked(odd[...]))


def face_kernel(even, odd, cat_even, cat_odd, part, out):
    out[...] = face_image(even, odd, cat_even, cat_odd, part)


def row_sum(values):
    return jnp.sum(values, axis=1, keepdims=True)


def last_face_kernel(even, odd, cat_even, cat_odd, part, first, second, early, out, sums, known):
    image = face_image(even, odd, cat_even, cat_odd, part)
    out[...] = image
    step = row_sum(early[0:1, :]) / row_sum(early[1:2, :])
    residual = first[...] - step * second[...]
    sums[...] = jnp.zeros_like(sums)
    sums[0:1, :] = jnp.sum(residual * image, axis=0, keepdims=True)
    known[...] = jnp.zeros_like(known)
    known[0:1, :] = jnp.sum(residual * residual, axis=0, keepdims=True)
    known[1:2, :] = jnp.sum(residual * second[...], axis=0, keepdims=True)


def step_kernel(early, known, late, out):
    step = row_sum(early[0:1, :]) / row_sum(early[1:2, :])
    out[...] = jnp.zeros_like(out)
    out[0:1, :] = known[0:1, :]
    out[1:2, :] = known[1:2, :] - step * late[0:1, :]


def last_kernel(start, first, second, third, early, final, solution, residual):
    norm_zero, product_zero = row_sum(early[0:1, :]), row_sum(early[1:2, :])
    norm_one, product_one = row_sum(final[0:1, :]), row_sum(final[1:2, :])
    step_zero = norm_zero / product_zero
    beta = norm_one / norm_zero
    step_one = norm_one / (product_one - beta * norm_one / step_zero)
    zeroth, once, twice = first[...], second[...], third[...]
    after = zeroth - step_zero * once
    image = once - step_zero * twice
    direction = after + beta * zeroth
    moved = image + beta * once
    solution[...] = start[...] + step_zero * zeroth + step_one * direction
    residual[...] = after - step_one * moved


def shards(
    start_factors,
    bin_factors,
    tile_speed,
    tile_weight,
    tile_cells,
    tile_count,
    inner_pairs,
    inner_weight,
    face_rows,
    face_count,
    face_weight,
):
    weights = tile_weight[0, 0]
    n_tiles, tile, _ = weights.shape
    inner = inner_weight[0, 0]
    n_inner = inner.shape[0]
    rows = face_rows[0, 0]
    n_face = rows.shape[1]
    own_rows, width = start_factors.shape
    n_bin = lax.axis_size("bin")
    part_rows = own_rows * n_bin
    bin_blocks = bin_factors.shape[0] // tile
    cells = tile_cells[0, 0].T
    pairs = inner_pairs[0, 0]

    face = face_weight[0, 0]
    face_even, face_odd = exchange_faces(face, face)

    rows_shape = (part_rows, width)
    tile_flops = 2 * tile * tile * width
    own_start, rhs, gain, bins_t, bins_s, inner_cat, diag, pick_hot, scatter_up, down_cat = call(
        functools.partial(prep_kernel, n_bin),
        [
            (start_factors.shape, f32),
            (rows_shape, f32),
            ((n_tiles, tile, tile), f32),
            ((bin_blocks, 2 * width, tile), bf16),
            ((bin_blocks, 2 * tile, width), bf16),
            ((n_inner, 2, tile, 3 * tile), bf16),
            (rows_shape, f32),
            ((2 * n_face, part_rows), bf16),
            ((part_rows, n_face), bf16),
            ((part_rows, 3 * n_face), bf16),
        ],
        start_factors, bin_factors, rows, face, inner, weights, tile_speed[0, 0],
        smem=(cells, tile_count, pairs, face_count[0]),
        hbm=True,
        scratch=[
            pltpu.VMEM(bin_factors.shape, bf16),
            pltpu.VMEM(rows.shape, jnp.int32),
            pltpu.VMEM(face.shape, f32),
            pltpu.VMEM(inner.shape, f32),
            pltpu.VMEM(weights.shape, bf16),
            pltpu.VMEM(weights.shape, bf16),
            pltpu.SemaphoreType.DMA((7,)),
        ],
        flops=n_tiles * tile_flops,
    )
    start_whole = gather_rows(start_factors, own_start)
    wide_cat = ((part_rows, 3 * n_face), bf16)
    cat_even, cat_odd = call(
        up_kernel, [wide_cat, wide_cat], face_even, face_odd, scatter_up, down_cat, flops=tile_flops
    )

    counts = face_count[0, 0].astype(f32)
    counts = jnp.where(lax.axis_index("seg") % 2 == 1, counts, counts[::-1])
    counts = jnp.broadcast_to(counts[:, None, None], (2, PAD, width)).reshape(2 * PAD, width)

    cat = ((part_rows, 2 * width), bf16)
    message = ((n_face, width), f32)
    sums = ((PAD, width), f32)

    def main(whole, whole_cat, diagonal, before=None):
        more = [] if before is None else [before]
        return call(
            main_kernel,
            [(rows_shape, f32)] + ([] if before is None else [sums]),
            whole, whole_cat, bins_t, bins_s, gain, inner_cat, diagonal, *more,
            smem=(cells, pairs),
            scratch=[pltpu.VMEM((n_tiles + 2 * n_inner, tile, width), f32)],
            flops=6 * n_tiles * tile_flops,
        )

    counted = ((n_face + PAD, width), f32)
    start_cat, even, odd = call(
        first_pick_kernel, [cat, counted, counted], start_whole, pick_hot, counts
    )
    even, odd = exchange_faces(even, odd)
    (part,) = main(start_whole, start_cat, diag)
    part, diag_all = call(
        first_face_kernel,
        [(rows_shape, f32), (rows_shape, f32)],
        even, odd, cat_even, cat_odd, part, start_whole, diag, rhs,
    )
    first = reduce_all(part)

    first_cat, even, odd = call(pick_kernel, [cat, message, message], first, pick_hot)
    even, odd = exchange_faces(even, odd)
    (part,) = main(first, first_cat, diag_all)
    (part,) = call(face_kernel, [(rows_shape, f32)], even, odd, cat_even, cat_odd, part)
    second = reduce_all(part)

    second_cat, even, odd = call(pick_kernel, [cat, message, message], second, pick_hot)
    even, odd = exchange_faces(even, odd)
    part, early = main(second, second_cat, diag_all, first)
    early = reduce_seg(early)
    part, late, known = call(
        last_face_kernel,
        [(rows_shape, f32), sums, sums],
        even, odd, cat_even, cat_odd, part, first, second, early,
    )
    third, late = reduce_own(part, late)
    (final,) = call(step_kernel, [sums], early, known, late)
    final = reduce_seg(final)
    offset = lax.axis_index("bin") * own_rows
    own = lambda whole: lax.dynamic_slice(whole, (offset, 0), (own_rows, width))
    return tuple(
        call(
            last_kernel,
            [(start_factors.shape, f32), (start_factors.shape, f32)],
            own_start, own(first), own(second), third, early, final,
        )
    )


def solution(mesh):
    return jax.shard_map(
        shards,
        mesh=mesh,
        in_specs=(
            P(("groups", "seg", "bin"), None),
            P(("groups", "bin"), None),
            P(("groups", "seg"), "bin", None, None, None),
            P(("groups", "seg"), "bin", None, None, None),
            P(("groups", "seg"), "bin", None, None),
            P(("groups", "seg"), "bin"),
            P(("groups", "seg"), "bin", None, None),
            P(("groups", "seg"), "bin", None, None, None),
            P(("groups", "seg"), "bin", None, None),
            P(("groups", "seg"), "bin", None),
            P(("groups", "seg"), "bin", None, None),
        ),
        out_specs=(P(("groups", "seg", "bin"), None), P(("groups", "seg", "bin"), None)),
        check_vma=False,
    )
```

```python
import functools

import jax
import jax.numpy as jnp
from jax import lax
from jax.experimental import pallas as pl
from jax.experimental.pallas import tpu as pltpu
from jax.sharding import PartitionSpec as P


PAD = 8
VMEM_BYTES = 16 << 20

f32 = jnp.float32
bf16 = jnp.bfloat16
ridge_weight = 0.5


def is_power_of_two(n):
    return n & (n - 1) == 0


def swap(x, axis, mask):
    n = lax.axis_size(axis)
    return lax.ppermute(x, axis, [(i, i ^ mask) for i in range(n)])


def bit_of(axis, mask):
    return (lax.axis_index(axis) & mask) != 0


def ordered(bit, mine, other, dim):
    first = jnp.where(bit, other, mine)
    second = jnp.where(bit, mine, other)
    return jnp.stack([first, second], dim)


def gather_rows(own, copy):
    n = lax.axis_size("bin")
    if not is_power_of_two(n):
        return lax.all_gather(own, "bin", axis=0, tiled=True)
    sent, held = own[None], copy[None]
    mask = n // 2
    while mask:
        got = swap(sent, "bin", mask)
        held = ordered(bit_of("bin", mask), held, got, 1)
        held = held.reshape((-1,) + own.shape)
        sent = held
        mask //= 2
    return held.reshape(-1, own.shape[-1])


def reduce_all(partial_rows):
    n = lax.axis_size("bin")
    if n == 1:
        return partial_rows
    if not is_power_of_two(n):
        return lax.psum(partial_rows, "bin")
    half = partial_rows.shape[0] // 2
    odd = bit_of("bin", 1)
    low, high = partial_rows[:half], partial_rows[half:]
    kept = jnp.where(odd, high, low) + swap(jnp.where(odd, low, high), "bin", 1)
    mask = 2
    while mask < n:
        kept = kept + swap(kept, "bin", mask)
        mask *= 2
    return ordered(odd, kept, swap(kept, "bin", 1), 0).reshape(partial_rows.shape)


def reduce_own(partial_rows, sums):
    n = lax.axis_size("bin")
    width = partial_rows.shape[1]
    if not is_power_of_two(n):
        own = lax.psum_scatter(partial_rows, "bin", scatter_dimension=0, tiled=True)
        return own, lax.psum(sums, "bin")
    blocks = partial_rows.reshape(n, -1, width)
    mask = 1
    while mask < n:
        split = blocks.reshape(-1, 2, blocks.shape[1], width)
        bit = bit_of("bin", mask)
        sent = jnp.where(bit, split[:, 0], split[:, 1])
        kept = jnp.where(bit, split[:, 1], split[:, 0])
        count = sent.shape[0] * sent.shape[1]
        message = jnp.concatenate([sent.reshape(count, width), sums], 0)
        got = swap(message, "bin", mask)
        blocks = kept + got[:count].reshape(kept.shape)
        sums = sums + got[count:]
        mask *= 2
    return blocks.reshape(-1, width), sums


def reduce_seg(sums):
    n = lax.axis_size("seg")
    if not is_power_of_two(n):
        return lax.psum(sums, "seg")
    mask = 1
    while mask < n:
        if mask * 2 < n:
            sums = sums + swap(sums, "seg", mask) + swap(sums, "seg", 2 * mask) + swap(sums, "seg", 3 * mask)
            mask *= 4
        else:
            sums = sums + swap(sums, "seg", mask)
            mask *= 2
    return sums


def face_pairs(first):
    n_seg, n_bin = lax.axis_size("seg"), lax.axis_size("bin")
    pairs = []
    for s in range(n_seg):
        other = s + 1 if (s - first) % 2 == 0 else s - 1
        for t in range(n_bin):
            if 0 <= other < n_seg:
                pairs.append((s * n_bin + t, other * n_bin + t))
            elif n_bin % 2 == 0:
                pairs.append((s * n_bin + t, s * n_bin + (t ^ 1)))
    return pairs


def exchange_faces(message_even, message_odd):
    got_even = lax.ppermute(message_even, ("seg", "bin"), face_pairs(0))
    got_odd = lax.ppermute(message_odd, ("seg", "bin"), face_pairs(1))
    return got_even, got_odd


def split(x):
    high = x.astype(bf16)
    return high, (x - high.astype(f32)).astype(bf16)


def dot(a, b):
    return lax.dot_general(a, b, (((1,), (0,)), ((), ())), preferred_element_type=f32)


def along(x):
    high, low = split(x)
    return jnp.concatenate([high, high, low], 1)


def stacked(x):
    high, low = split(x)
    return jnp.concatenate([high, low, high], 0)


def call(kernel, outs, *operands, smem=(), scratch=(), flops=0):
    in_smem = pl.BlockSpec(memory_space=pltpu.SMEM)
    in_vmem = pl.BlockSpec(memory_space=pltpu.VMEM)
    nbytes = sum(o.size * o.dtype.itemsize for o in operands)
    return pl.pallas_call(
        kernel,
        out_shape=[jax.ShapeDtypeStruct(shape, kind) for shape, kind in outs],
        in_specs=[in_smem] * len(smem) + [in_vmem] * len(operands),
        out_specs=[in_vmem] * len(outs),
        scratch_shapes=scratch,
        compiler_params=pltpu.CompilerParams(vmem_limit_bytes=VMEM_BYTES),
        cost_estimate=pl.CostEstimate(flops=flops, bytes_accessed=nbytes, transcendentals=0),
    )(*smem, *operands)


def block_at(index, size):
    return pl.ds(pl.multiple_of(index * size, size), size)


def hot_kernel(faces, rows, own, pick_hot, scatter_low, scatter_up, counts, copy):
    copy[...] = own[...]
    part_rows, n_face = scatter_up.shape
    is_odd = lax.axis_index("seg") % 2 == 1
    slots = lax.broadcasted_iota(jnp.int32, (1, n_face), 1)
    ids = lax.broadcasted_iota(jnp.int32, (part_rows, n_face), 0)
    hots = []
    for side in range(2):
        listed = jnp.where(slots < faces[0, side], rows[side:side + 1, :], -1)
        hots.append((ids == listed).astype(f32))
    scatter_low[...] = hots[0].astype(bf16)
    scatter_up[...] = hots[1].astype(bf16)
    low_t, up_t = hots[0].T.astype(bf16), hots[1].T.astype(bf16)
    pick_hot[0:n_face, :] = jnp.where(is_odd, low_t, up_t)
    pick_hot[n_face:, :] = jnp.where(is_odd, up_t, low_t)
    low_count, up_count = faces[0, 0], faces[0, 1]
    shape = (PAD, counts.shape[1])
    counts[0:PAD, :] = jnp.full(shape, jnp.where(is_odd, low_count, up_count), jnp.int32).astype(f32)
    counts[PAD:, :] = jnp.full(shape, jnp.where(is_odd, up_count, low_count), jnp.int32).astype(f32)


def prep_kernel(n_bin, cells, count, pairs, bins, face, inner, weights, speeds, scatter_low,
                rhs, gain, bins_t, bins_s, inner_cat, diag, down_cat):
    n_tiles, tile, _ = weights.shape
    width = bins.shape[1]
    is_first = lax.axis_index("seg") == 0
    rhs[...] = jnp.zeros_like(rhs)
    diag[...] = jnp.full(diag.shape, ridge_weight / n_bin, f32)
    high, low = split(jnp.where(is_first, 0.0, face[...]))
    hot = scatter_low[...]
    high = dot(hot, high).astype(bf16)
    low = dot(hot, low).astype(bf16)
    down_cat[...] = jnp.concatenate([high, high, low], 1)
    for k in range(bins.shape[0] // tile):
        block = bins[k * tile:(k + 1) * tile, :]
        flipped = block.astype(f32).T.astype(bf16)
        bins_t[k] = jnp.concatenate([flipped, flipped], 0)
        bins_s[k] = jnp.concatenate([block, block], 0)
    for j in range(inner.shape[0]):
        block = inner[j]
        flipped = block.T
        inner_cat[j, 0] = along(block)
        inner_cat[j, 1] = along(flipped)
        for side, matrix in enumerate((block, flipped)):
            degree = jnp.sum(matrix, axis=1, keepdims=True)
            diag[block_at(pairs[j, side], tile), :] += jnp.broadcast_to(degree, (tile, width))
    for k in range(n_tiles):
        wide = weights[k].astype(f32)
        live = jnp.where(k < count[0, 0], 1.0, 0.0).astype(f32)
        gain[k] = wide * live
        weighted = (wide * speeds[k].astype(f32)).astype(bf16)
        terms = dot(weighted, bins[block_at(cells[1, k], tile), :]) * live
        rhs[block_at(cells[0, k], tile), :] += terms


def up_kernel(face_even, face_odd, scatter_up, down_cat, cat_even, cat_odd):
    index = lax.axis_index("seg")
    is_odd = index % 2 == 1
    is_last = index == lax.axis_size("seg") - 1
    following = jnp.where(is_odd, face_odd[...], face_even[...])
    high, low = split(jnp.where(is_last, 0.0, following).T)
    hot = scatter_up[...]
    high = dot(hot, high).astype(bf16)
    low = dot(hot, low).astype(bf16)
    up = jnp.concatenate([high, high, low], 1)
    down = down_cat[...]
    cat_even[...] = jnp.where(is_odd, down, up)
    cat_odd[...] = jnp.where(is_odd, up, down)


def pick(whole, pick_hot, whole_cat):
    width = whole.shape[1]
    high, low = split(whole[...])
    cat = jnp.concatenate([high, low], 1)
    whole_cat[...] = cat
    picked = dot(pick_hot[...], cat)
    return picked[:, :width] + picked[:, width:]


def first_pick_kernel(whole, pick_hot, counts, whole_cat, even, odd):
    picked = pick(whole, pick_hot, whole_cat)
    n_face = picked.shape[0] // 2
    even[0:n_face, :] = picked[:n_face]
    odd[0:n_face, :] = picked[n_face:]
    even[n_face:, :] = counts[0:PAD, :]
    odd[n_face:, :] = counts[PAD:, :]


def pick_kernel(whole, pick_hot, whole_cat, even, odd):
    picked = pick(whole, pick_hot, whole_cat)
    n_face = picked.shape[0] // 2
    even[...] = picked[:n_face]
    odd[...] = picked[n_face:]


def main_kernel(cells, pairs, whole, whole_cat, bins_t, bins_s, gain, inner_cat, diag, *refs):
    if len(refs) == 4:
        before, out, sums, terms = refs
        now, old = whole[...], before[...]
        sums[...] = jnp.zeros_like(sums)
        sums[0:1, :] = jnp.sum(old * old, axis=0, keepdims=True)
        sums[1:2, :] = jnp.sum(old * now, axis=0, keepdims=True)
    else:
        out, terms = refs
    n_tiles, tile, _ = gain.shape
    width = whole.shape[1]
    for k in range(n_tiles):
        scores = dot(whole_cat[block_at(cells[0, k], tile), :], bins_t[cells[1, k]]) * gain[k]
        high, low = split(scores)
        terms[k] = dot(jnp.concatenate([high, low], 1), bins_s[cells[1, k]])
    n_inner = inner_cat.shape[0]
    for j in range(n_inner):
        for side in range(2):
            other = whole_cat[block_at(pairs[j, 1 - side], tile), :]
            high, low = other[:, :width], other[:, width:]
            terms[n_tiles + 2 * j + side] = -dot(inner_cat[j, side], jnp.concatenate([high, low, high], 0))
    out[...] = diag[...] * whole[...]
    for k in range(n_tiles):
        out[block_at(cells[0, k], tile), :] += terms[k]
    for j in range(n_inner):
        for side in range(2):
            out[block_at(pairs[j, side], tile), :] += terms[n_tiles + 2 * j + side]


def first_face_kernel(even, odd, cat_even, cat_odd, part, whole, diag, rhs, out, diag_all):
    n_face = cat_even.shape[1] // 3
    width = part.shape[1]
    slots = lax.broadcasted_iota(jnp.int32, (n_face, width), 0).astype(f32)
    both = jnp.zeros((part.shape[0], 2 * width), f32)
    for got, cat in ((even, cat_even), (odd, cat_odd)):
        live = jnp.where(slots < got[n_face:n_face + 1, :], 1.0, 0.0).astype(bf16)
        seen = jnp.concatenate([live, jnp.zeros_like(live), live], 0)
        both = both + dot(cat[...], jnp.concatenate([stacked(got[0:n_face, :]), seen], 1))
    degree = both[:, width:]
    diag_all[...] = diag[...] + degree
    out[...] = rhs[...] - (part[...] + degree * whole[...] - both[:, :width])


def face_image(even, odd, cat_even, cat_odd, part):
    return part[...] - dot(cat_even[...], stacked(even[...])) - dot(cat_odd[...], stacked(odd[...]))


def face_kernel(even, odd, cat_even, cat_odd, part, out):
    out[...] = face_image(even, odd, cat_even, cat_odd, part)


def row_sum(values):
    return jnp.sum(values, axis=1, keepdims=True)


def last_face_kernel(even, odd, cat_even, cat_odd, part, first, second, early, out, sums, known):
    image = face_image(even, odd, cat_even, cat_odd, part)
    out[...] = image
    step = row_sum(early[0:1, :]) / row_sum(early[1:2, :])
    residual = first[...] - step * second[...]
    sums[...] = jnp.zeros_like(sums)
    sums[0:1, :] = jnp.sum(residual * image, axis=0, keepdims=True)
    known[...] = jnp.zeros_like(known)
    known[0:1, :] = jnp.sum(residual * residual, axis=0, keepdims=True)
    known[1:2, :] = jnp.sum(residual * second[...], axis=0, keepdims=True)


def step_kernel(early, known, late, out):
    step = row_sum(early[0:1, :]) / row_sum(early[1:2, :])
    out[...] = jnp.zeros_like(out)
    out[0:1, :] = known[0:1, :]
    out[1:2, :] = known[1:2, :] - step * late[0:1, :]


def last_kernel(start, first, second, third, early, final, solution, residual):
    norm_zero, product_zero = row_sum(early[0:1, :]), row_sum(early[1:2, :])
    norm_one, product_one = row_sum(final[0:1, :]), row_sum(final[1:2, :])
    step_zero = norm_zero / product_zero
    beta = norm_one / norm_zero
    step_one = norm_one / (product_one - beta * norm_one / step_zero)
    zeroth, once, twice = first[...], second[...], third[...]
    after = zeroth - step_zero * once
    image = once - step_zero * twice
    direction = after + beta * zeroth
    moved = image + beta * once
    solution[...] = start[...] + step_zero * zeroth + step_one * direction
    residual[...] = after - step_one * moved


def shards(
    start_factors,
    bin_factors,
    tile_speed,
    tile_weight,
    tile_cells,
    tile_count,
    inner_pairs,
    inner_weight,
    face_rows,
    face_count,
    face_weight,
):
    weights = tile_weight[0, 0]
    n_tiles, tile, _ = weights.shape
    inner = inner_weight[0, 0]
    n_inner = inner.shape[0]
    rows = face_rows[0, 0]
    n_face = rows.shape[1]
    own_rows, width = start_factors.shape
    n_bin = lax.axis_size("bin")
    part_rows = own_rows * n_bin
    bin_blocks = bin_factors.shape[0] // tile
    cells = tile_cells[0, 0].T
    pairs = inner_pairs[0, 0]

    face = face_weight[0, 0]
    face_even, face_odd = exchange_faces(face, face)

    rows_shape = (part_rows, width)
    tile_flops = 2 * tile * tile * width
    pick_hot, scatter_low, scatter_up, counts, own_start = call(
        hot_kernel,
        [
            ((2 * n_face, part_rows), bf16),
            ((part_rows, n_face), bf16),
            ((part_rows, n_face), bf16),
            ((2 * PAD, width), f32),
            (start_factors.shape, f32),
        ],
        rows, start_factors,
        smem=(face_count[0],),
        flops=tile_flops,
    )
    start_whole = gather_rows(start_factors, own_start)
    rhs, gain, bins_t, bins_s, inner_cat, diag, down_cat = call(
        functools.partial(prep_kernel, n_bin),
        [
            (rows_shape, f32),
            ((n_tiles, tile, tile), f32),
            ((bin_blocks, 2 * width, tile), bf16),
            ((bin_blocks, 2 * tile, width), bf16),
            ((n_inner, 2, tile, 3 * tile), bf16),
            (rows_shape, f32),
            ((part_rows, 3 * n_face), bf16),
        ],
        bin_factors, face, inner, weights, tile_speed[0, 0], scatter_low,
        smem=(cells, tile_count, pairs),
        flops=3 * n_tiles * tile_flops,
    )
    wide_cat = ((part_rows, 3 * n_face), bf16)
    cat_even, cat_odd = call(
        up_kernel, [wide_cat, wide_cat], face_even, face_odd, scatter_up, down_cat, flops=tile_flops
    )

    cat = ((part_rows, 2 * width), bf16)
    message = ((n_face, width), f32)
    sums = ((PAD, width), f32)

    def main(whole, whole_cat, diagonal, before=None):
        more = [] if before is None else [before]
        return call(
            main_kernel,
            [(rows_shape, f32)] + ([] if before is None else [sums]),
            whole, whole_cat, bins_t, bins_s, gain, inner_cat, diagonal, *more,
            smem=(cells, pairs),
            scratch=[pltpu.VMEM((n_tiles + 2 * n_inner, tile, width), f32)],
            flops=6 * n_tiles * tile_flops,
        )

    counted = ((n_face + PAD, width), f32)
    start_cat, even, odd = call(
        first_pick_kernel, [cat, counted, counted], start_whole, pick_hot, counts
    )
    even, odd = exchange_faces(even, odd)
    (part,) = main(start_whole, start_cat, diag)
    part, diag_all = call(
        first_face_kernel,
        [(rows_shape, f32), (rows_shape, f32)],
        even, odd, cat_even, cat_odd, part, start_whole, diag, rhs,
    )
    first = reduce_all(part)

    first_cat, even, odd = call(pick_kernel, [cat, message, message], first, pick_hot)
    even, odd = exchange_faces(even, odd)
    (part,) = main(first, first_cat, diag_all)
    (part,) = call(face_kernel, [(rows_shape, f32)], even, odd, cat_even, cat_odd, part)
    second = reduce_all(part)

    second_cat, even, odd = call(pick_kernel, [cat, message, message], second, pick_hot)
    even, odd = exchange_faces(even, odd)
    part, early = main(second, second_cat, diag_all, first)
    early = reduce_seg(early)
    part, late, known = call(
        last_face_kernel,
        [(rows_shape, f32), sums, sums],
        even, odd, cat_even, cat_odd, part, first, second, early,
    )
    third, late = reduce_own(part, late)
    (final,) = call(step_kernel, [sums], early, known, late)
    final = reduce_seg(final)
    offset = lax.axis_index("bin") * own_rows
    own = lambda whole: lax.dynamic_slice(whole, (offset, 0), (own_rows, width))
    return tuple(
        call(
            last_kernel,
            [(start_factors.shape, f32), (start_factors.shape, f32)],
            own_start, own(first), own(second), third, early, final,
        )
    )


def solution(mesh):
    return jax.shard_map(
        shards,
        mesh=mesh,
        in_specs=(
            P(("groups", "seg", "bin"), None),
            P(("groups", "bin"), None),
            P(("groups", "seg"), "bin", None, None, None),
            P(("groups", "seg"), "bin", None, None, None),
            P(("groups", "seg"), "bin", None, None),
            P(("groups", "seg"), "bin"),
            P(("groups", "seg"), "bin", None, None),
            P(("groups", "seg"), "bin", None, None, None),
            P(("groups", "seg"), "bin", None, None),
            P(("groups", "seg"), "bin", None),
            P(("groups", "seg"), "bin", None, None),
        ),
        out_specs=(P(("groups", "seg", "bin"), None), P(("groups", "seg", "bin"), None)),
        check_vma=False,
    )
```

```python
import functools

import jax
import jax.numpy as jnp
from jax import lax
from jax.experimental import pallas as pl
from jax.experimental.pallas import tpu as pltpu
from jax.sharding import PartitionSpec as P


PAD = 8
VMEM_BYTES = 16 << 20

f32 = jnp.float32
bf16 = jnp.bfloat16
ridge_weight = 0.5


def is_power_of_two(n):
    return n & (n - 1) == 0


def swap(x, axis, mask):
    n = lax.axis_size(axis)
    return lax.ppermute(x, axis, [(i, i ^ mask) for i in range(n)])


def bit_of(axis, mask):
    return (lax.axis_index(axis) & mask) != 0


def ordered(bit, mine, other, dim):
    first = jnp.where(bit, other, mine)
    second = jnp.where(bit, mine, other)
    return jnp.stack([first, second], dim)


def gather_rows(own, copy):
    n = lax.axis_size("bin")
    if not is_power_of_two(n):
        return lax.all_gather(own, "bin", axis=0, tiled=True)
    sent, held = own[None], copy[None]
    mask = n // 2
    while mask:
        got = swap(sent, "bin", mask)
        held = ordered(bit_of("bin", mask), held, got, 1)
        held = held.reshape((-1,) + own.shape)
        sent = held
        mask //= 2
    return held.reshape(-1, own.shape[-1])


def reduce_all(partial_rows):
    n = lax.axis_size("bin")
    if n == 1:
        return partial_rows
    if not is_power_of_two(n):
        return lax.psum(partial_rows, "bin")
    half = partial_rows.shape[0] // 2
    odd = bit_of("bin", 1)
    low, high = partial_rows[:half], partial_rows[half:]
    kept = jnp.where(odd, high, low) + swap(jnp.where(odd, low, high), "bin", 1)
    mask = 2
    while mask < n:
        kept = kept + swap(kept, "bin", mask)
        mask *= 2
    return ordered(odd, kept, swap(kept, "bin", 1), 0).reshape(partial_rows.shape)


def reduce_own(partial_rows, sums):
    n = lax.axis_size("bin")
    width = partial_rows.shape[1]
    if not is_power_of_two(n):
        own = lax.psum_scatter(partial_rows, "bin", scatter_dimension=0, tiled=True)
        return own, lax.psum(sums, "bin")
    blocks = partial_rows.reshape(n, -1, width)
    mask = 1
    while mask < n:
        split = blocks.reshape(-1, 2, blocks.shape[1], width)
        bit = bit_of("bin", mask)
        sent = jnp.where(bit, split[:, 0], split[:, 1])
        kept = jnp.where(bit, split[:, 1], split[:, 0])
        count = sent.shape[0] * sent.shape[1]
        message = jnp.concatenate([sent.reshape(count, width), sums], 0)
        got = swap(message, "bin", mask)
        blocks = kept + got[:count].reshape(kept.shape)
        sums = sums + got[count:]
        mask *= 2
    return blocks.reshape(-1, width), sums


def reduce_seg(sums):
    n = lax.axis_size("seg")
    if not is_power_of_two(n):
        return lax.psum(sums, "seg")
    mask = 1
    while mask < n:
        if mask * 2 < n:
            sums = sums + swap(sums, "seg", mask) + swap(sums, "seg", 2 * mask) + swap(sums, "seg", 3 * mask)
            mask *= 4
        else:
            sums = sums + swap(sums, "seg", mask)
            mask *= 2
    return sums


def face_pairs(first):
    n_seg, n_bin = lax.axis_size("seg"), lax.axis_size("bin")
    pairs = []
    for s in range(n_seg):
        other = s + 1 if (s - first) % 2 == 0 else s - 1
        for t in range(n_bin):
            if 0 <= other < n_seg:
                pairs.append((s * n_bin + t, other * n_bin + t))
            elif n_bin % 2 == 0:
                pairs.append((s * n_bin + t, s * n_bin + (t ^ 1)))
    return pairs


def exchange_faces(message_even, message_odd):
    got_even = lax.ppermute(message_even, ("seg", "bin"), face_pairs(0))
    got_odd = lax.ppermute(message_odd, ("seg", "bin"), face_pairs(1))
    return got_even, got_odd


def split(x):
    high = x.astype(bf16)
    return high, (x - high.astype(f32)).astype(bf16)


def dot(a, b):
    return lax.dot_general(a, b, (((1,), (0,)), ((), ())), preferred_element_type=f32)


def along(x):
    high, low = split(x)
    return jnp.concatenate([high, high, low], 1)


def stacked(x):
    high, low = split(x)
    return jnp.concatenate([high, low, high], 0)


def call(kernel, outs, *operands, smem=(), scratch=(), flops=0):
    in_smem = pl.BlockSpec(memory_space=pltpu.SMEM)
    in_vmem = pl.BlockSpec(memory_space=pltpu.VMEM)
    nbytes = sum(o.size * o.dtype.itemsize for o in operands)
    return pl.pallas_call(
        kernel,
        out_shape=[jax.ShapeDtypeStruct(shape, kind) for shape, kind in outs],
        in_specs=[in_smem] * len(smem) + [in_vmem] * len(operands),
        out_specs=[in_vmem] * len(outs),
        scratch_shapes=scratch,
        compiler_params=pltpu.CompilerParams(vmem_limit_bytes=VMEM_BYTES),
        cost_estimate=pl.CostEstimate(flops=flops, bytes_accessed=nbytes, transcendentals=0),
    )(*smem, *operands)


def block_at(index, size):
    return pl.ds(pl.multiple_of(index * size, size), size)


def hot_kernel(faces, rows, own, pick_hot, scatter_low, scatter_up, counts, copy):
    copy[...] = own[...]
    part_rows, n_face = scatter_up.shape
    is_odd = lax.axis_index("seg") % 2 == 1
    slots = lax.broadcasted_iota(jnp.int32, (1, n_face), 1)
    ids = lax.broadcasted_iota(jnp.int32, (part_rows, n_face), 0)
    hots = []
    for side in range(2):
        listed = jnp.where(slots < faces[0, side], rows[side:side + 1, :], -1)
        hots.append((ids == listed).astype(f32))
    scatter_low[...] = hots[0].astype(bf16)
    scatter_up[...] = hots[1].astype(bf16)
    low_t, up_t = hots[0].T.astype(bf16), hots[1].T.astype(bf16)
    pick_hot[0:n_face, :] = jnp.where(is_odd, low_t, up_t)
    pick_hot[n_face:, :] = jnp.where(is_odd, up_t, low_t)
    low_count, up_count = faces[0, 0], faces[0, 1]
    shape = (PAD, counts.shape[1])
    counts[0:PAD, :] = jnp.full(shape, jnp.where(is_odd, low_count, up_count), jnp.int32).astype(f32)
    counts[PAD:, :] = jnp.full(shape, jnp.where(is_odd, up_count, low_count), jnp.int32).astype(f32)


def prep_kernel(n_bin, cells, count, pairs, bins, face, inner, weights, speeds, scatter_low,
                rhs, gain, bins_t, bins_s, inner_cat, diag, down_cat):
    n_tiles, tile, _ = weights.shape
    width = bins.shape[1]
    is_first = lax.axis_index("seg") == 0
    rhs[...] = jnp.zeros_like(rhs)
    diag[...] = jnp.full(diag.shape, ridge_weight / n_bin, f32)
    high, low = split(jnp.where(is_first, 0.0, face[...]))
    hot = scatter_low[...]
    high = dot(hot, high).astype(bf16)
    low = dot(hot, low).astype(bf16)
    down_cat[...] = jnp.concatenate([high, high, low], 1)
    for k in range(bins.shape[0] // tile):
        block = bins[k * tile:(k + 1) * tile, :]
        flipped = block.astype(f32).T.astype(bf16)
        bins_t[k] = jnp.concatenate([flipped, flipped], 0)
        bins_s[k] = jnp.concatenate([block, block], 0)
    for j in range(inner.shape[0]):
        block = inner[j]
        flipped = block.T
        inner_cat[j, 0] = along(block)
        inner_cat[j, 1] = along(flipped)
        for side, matrix in enumerate((block, flipped)):
            degree = jnp.sum(matrix, axis=1, keepdims=True)
            diag[block_at(pairs[j, side], tile), :] += jnp.broadcast_to(degree, (tile, width))
    for k in range(n_tiles):
        wide = weights[k].astype(f32)
        live = jnp.where(k < count[0, 0], 1.0, 0.0).astype(f32)
        gain[k] = wide * live
        weighted = (wide * speeds[k].astype(f32)).astype(bf16)
        terms = dot(weighted, bins[block_at(cells[1, k], tile), :]) * live
        rhs[block_at(cells[0, k], tile), :] += terms


def up_kernel(face_even, face_odd, scatter_up, down_cat, cat_even, cat_odd):
    index = lax.axis_index("seg")
    is_odd = index % 2 == 1
    is_last = index == lax.axis_size("seg") - 1
    following = jnp.where(is_odd, face_odd[...], face_even[...])
    high, low = split(jnp.where(is_last, 0.0, following).T)
    hot = scatter_up[...]
    high = dot(hot, high).astype(bf16)
    low = dot(hot, low).astype(bf16)
    up = jnp.concatenate([high, high, low], 1)
    down = down_cat[...]
    cat_even[...] = jnp.where(is_odd, down, up)
    cat_odd[...] = jnp.where(is_odd, up, down)


def pick(whole, pick_hot, whole_cat):
    width = whole.shape[1]
    high, low = split(whole[...])
    cat = jnp.concatenate([high, low], 1)
    whole_cat[...] = cat
    picked = dot(pick_hot[...], cat)
    return picked[:, :width] + picked[:, width:]


def first_pick_kernel(whole, pick_hot, counts, whole_cat, even, odd):
    picked = pick(whole, pick_hot, whole_cat)
    n_face = picked.shape[0] // 2
    even[0:n_face, :] = picked[:n_face]
    odd[0:n_face, :] = picked[n_face:]
    even[n_face:, :] = counts[0:PAD, :]
    odd[n_face:, :] = counts[PAD:, :]


def pick_kernel(whole, pick_hot, *refs):
    if len(refs) == 5:
        before, whole_cat, even, odd, sums = refs
        now, old = whole[...], before[...]
        sums[...] = jnp.zeros_like(sums)
        sums[0:1, :] = jnp.sum(old * old, axis=0, keepdims=True)
        sums[1:2, :] = jnp.sum(old * now, axis=0, keepdims=True)
    else:
        whole_cat, even, odd = refs
    picked = pick(whole, pick_hot, whole_cat)
    n_face = picked.shape[0] // 2
    even[...] = picked[:n_face]
    odd[...] = picked[n_face:]


def main_kernel(cells, pairs, whole, whole_cat, bins_t, bins_s, gain, inner_cat, diag, out, terms):
    n_tiles, tile, _ = gain.shape
    width = whole.shape[1]
    for k in range(n_tiles):
        scores = dot(whole_cat[block_at(cells[0, k], tile), :], bins_t[cells[1, k]]) * gain[k]
        high, low = split(scores)
        terms[k] = dot(jnp.concatenate([high, low], 1), bins_s[cells[1, k]])
    n_inner = inner_cat.shape[0]
    for j in range(n_inner):
        for side in range(2):
            other = whole_cat[block_at(pairs[j, 1 - side], tile), :]
            high, low = other[:, :width], other[:, width:]
            terms[n_tiles + 2 * j + side] = -dot(inner_cat[j, side], jnp.concatenate([high, low, high], 0))
    out[...] = diag[...] * whole[...]
    for k in range(n_tiles):
        out[block_at(cells[0, k], tile), :] += terms[k]
    for j in range(n_inner):
        for side in range(2):
            out[block_at(pairs[j, side], tile), :] += terms[n_tiles + 2 * j + side]


def first_face_kernel(even, odd, cat_even, cat_odd, part, whole, diag, rhs, out, diag_all):
    n_face = cat_even.shape[1] // 3
    width = part.shape[1]
    slots = lax.broadcasted_iota(jnp.int32, (n_face, width), 0).astype(f32)
    both = jnp.zeros((part.shape[0], 2 * width), f32)
    for got, cat in ((even, cat_even), (odd, cat_odd)):
        live = jnp.where(slots < got[n_face:n_face + 1, :], 1.0, 0.0).astype(bf16)
        seen = jnp.concatenate([live, jnp.zeros_like(live), live], 0)
        both = both + dot(cat[...], jnp.concatenate([stacked(got[0:n_face, :]), seen], 1))
    degree = both[:, width:]
    diag_all[...] = diag[...] + degree
    out[...] = rhs[...] - (part[...] + degree * whole[...] - both[:, :width])


def face_image(even, odd, cat_even, cat_odd, part):
    return part[...] - dot(cat_even[...], stacked(even[...])) - dot(cat_odd[...], stacked(odd[...]))


def face_kernel(even, odd, cat_even, cat_odd, part, out):
    out[...] = face_image(even, odd, cat_even, cat_odd, part)


def row_sum(values):
    return jnp.sum(values, axis=1, keepdims=True)


def last_face_kernel(even, odd, cat_even, cat_odd, part, first, second, early, out, sums, known):
    image = face_image(even, odd, cat_even, cat_odd, part)
    out[...] = image
    step = row_sum(early[0:1, :]) / row_sum(early[1:2, :])
    residual = first[...] - step * second[...]
    sums[...] = jnp.zeros_like(sums)
    sums[0:1, :] = jnp.sum(residual * image, axis=0, keepdims=True)
    known[...] = jnp.zeros_like(known)
    known[0:1, :] = jnp.sum(residual * residual, axis=0, keepdims=True)
    known[1:2, :] = jnp.sum(residual * second[...], axis=0, keepdims=True)


def step_kernel(early, known, late, out):
    step = row_sum(early[0:1, :]) / row_sum(early[1:2, :])
    out[...] = jnp.zeros_like(out)
    out[0:1, :] = known[0:1, :]
    out[1:2, :] = known[1:2, :] - step * late[0:1, :]


def last_kernel(start, first, second, third, early, final, solution, residual):
    norm_zero, product_zero = row_sum(early[0:1, :]), row_sum(early[1:2, :])
    norm_one, product_one = row_sum(final[0:1, :]), row_sum(final[1:2, :])
    step_zero = norm_zero / product_zero
    beta = norm_one / norm_zero
    step_one = norm_one / (product_one - beta * norm_one / step_zero)
    zeroth, once, twice = first[...], second[...], third[...]
    after = zeroth - step_zero * once
    image = once - step_zero * twice
    direction = after + beta * zeroth
    moved = image + beta * once
    solution[...] = start[...] + step_zero * zeroth + step_one * direction
    residual[...] = after - step_one * moved


def shards(
    start_factors,
    bin_factors,
    tile_speed,
    tile_weight,
    tile_cells,
    tile_count,
    inner_pairs,
    inner_weight,
    face_rows,
    face_count,
    face_weight,
):
    weights = tile_weight[0, 0]
    n_tiles, tile, _ = weights.shape
    inner = inner_weight[0, 0]
    n_inner = inner.shape[0]
    rows = face_rows[0, 0]
    n_face = rows.shape[1]
    own_rows, width = start_factors.shape
    n_bin = lax.axis_size("bin")
    part_rows = own_rows * n_bin
    bin_blocks = bin_factors.shape[0] // tile
    cells = tile_cells[0, 0].T
    pairs = inner_pairs[0, 0]

    face = face_weight[0, 0]
    face_even, face_odd = exchange_faces(face, face)

    rows_shape = (part_rows, width)
    tile_flops = 2 * tile * tile * width
    pick_hot, scatter_low, scatter_up, counts, own_start = call(
        hot_kernel,
        [
            ((2 * n_face, part_rows), bf16),
            ((part_rows, n_face), bf16),
            ((part_rows, n_face), bf16),
            ((2 * PAD, width), f32),
            (start_factors.shape, f32),
        ],
        rows, start_factors,
        smem=(face_count[0],),
        flops=tile_flops,
    )
    start_whole = gather_rows(start_factors, own_start)
    rhs, gain, bins_t, bins_s, inner_cat, diag, down_cat = call(
        functools.partial(prep_kernel, n_bin),
        [
            (rows_shape, f32),
            ((n_tiles, tile, tile), f32),
            ((bin_blocks, 2 * width, tile), bf16),
            ((bin_blocks, 2 * tile, width), bf16),
            ((n_inner, 2, tile, 3 * tile), bf16),
            (rows_shape, f32),
            ((part_rows, 3 * n_face), bf16),
        ],
        bin_factors, face, inner, weights, tile_speed[0, 0], scatter_low,
        smem=(cells, tile_count, pairs),
        flops=3 * n_tiles * tile_flops,
    )
    wide_cat = ((part_rows, 3 * n_face), bf16)
    cat_even, cat_odd = call(
        up_kernel, [wide_cat, wide_cat], face_even, face_odd, scatter_up, down_cat, flops=tile_flops
    )

    cat = ((part_rows, 2 * width), bf16)
    message = ((n_face, width), f32)
    sums = ((PAD, width), f32)

    def main(whole, whole_cat, diagonal):
        (part,) = call(
            main_kernel,
            [(rows_shape, f32)],
            whole, whole_cat, bins_t, bins_s, gain, inner_cat, diagonal,
            smem=(cells, pairs),
            scratch=[pltpu.VMEM((n_tiles + 2 * n_inner, tile, width), f32)],
            flops=6 * n_tiles * tile_flops,
        )
        return part

    counted = ((n_face + PAD, width), f32)
    start_cat, even, odd = call(
        first_pick_kernel, [cat, counted, counted], start_whole, pick_hot, counts
    )
    even, odd = exchange_faces(even, odd)
    part = main(start_whole, start_cat, diag)
    part, diag_all = call(
        first_face_kernel,
        [(rows_shape, f32), (rows_shape, f32)],
        even, odd, cat_even, cat_odd, part, start_whole, diag, rhs,
    )
    first = reduce_all(part)

    first_cat, even, odd = call(pick_kernel, [cat, message, message], first, pick_hot)
    even, odd = exchange_faces(even, odd)
    part = main(first, first_cat, diag_all)
    (part,) = call(face_kernel, [(rows_shape, f32)], even, odd, cat_even, cat_odd, part)
    second = reduce_all(part)

    second_cat, even, odd, early = call(
        pick_kernel, [cat, message, message, sums], second, pick_hot, first
    )
    even, odd = exchange_faces(even, odd)
    part = main(second, second_cat, diag_all)
    early = reduce_seg(early)
    part, late, known = call(
        last_face_kernel,
        [(rows_shape, f32), sums, sums],
        even, odd, cat_even, cat_odd, part, first, second, early,
    )
    third, late = reduce_own(part, late)
    (final,) = call(step_kernel, [sums], early, known, late)
    final = reduce_seg(final)
    offset = lax.axis_index("bin") * own_rows
    own = lambda whole: lax.dynamic_slice(whole, (offset, 0), (own_rows, width))
    return tuple(
        call(
            last_kernel,
            [(start_factors.shape, f32), (start_factors.shape, f32)],
            own_start, own(first), own(second), third, early, final,
        )
    )


def solution(mesh):
    return jax.shard_map(
        shards,
        mesh=mesh,
        in_specs=(
            P(("groups", "seg", "bin"), None),
            P(("groups", "bin"), None),
            P(("groups", "seg"), "bin", None, None, None),
            P(("groups", "seg"), "bin", None, None, None),
            P(("groups", "seg"), "bin", None, None),
            P(("groups", "seg"), "bin"),
            P(("groups", "seg"), "bin", None, None),
            P(("groups", "seg"), "bin", None, None, None),
            P(("groups", "seg"), "bin", None, None),
            P(("groups", "seg"), "bin", None),
            P(("groups", "seg"), "bin", None, None),
        ),
        out_specs=(P(("groups", "seg", "bin"), None), P(("groups", "seg", "bin"), None)),
        check_vma=False,
    )
```
